8 devices in a mesh: batch: 1 (over z), dap: 8 (over y, x, core).
Axes of the slice: x: 2, y: 2, z: 1, core: 2. Of those that a mesh axis runs over, the one named last changes fastest.
Arguments:
- z_pair: bfloat16 [256, 256, 128], P(('batch', 'dap'))
- msa_feat: bfloat16 [512, 256, 64], P(None, ('batch', 'dap'))
- ln_scale: bfloat16 [64], replicated
- ln_offset: bfloat16 [64], replicated
- w_a: bfloat16 [64, 32], replicated
- b_a: bfloat16 [32], replicated
- w_b: bfloat16 [64, 32], replicated
- b_b: bfloat16 [32], replicated
- w_out: bfloat16 [1024, 128], replicated
- b_out: bfloat16 [128], replicated
Outputs:
- output: bfloat16 [256, 256, 128], P(('batch', 'dap'))
All inputs are finite; a program needn't handle non-finite values.
Results may differ from the reference program's by a relative error of at most 0.001.
Values are sent between devices in bfloat16 or wider.
A program may use at most 1 GiB of HBM per device.

```python
import jax
import jax.numpy as jnp
from jax import lax

MSA_ROWS = 512
N_RES = 256
MSA_DIM = 64
HID_DIM = 32
PAIR_DIM = 128
LOW_RANK = 4

LN_EPS = 1e-5
ROW_TILE = min(N_RES, max(1, 8192 // N_RES))


def normal_draw(rng_key, shape_in, scale_in):
    return jax.random.normal(rng_key, shape_in, jnp.float32) * scale_in


def setup_inputs(seed: int = 0, part: int = 0) -> dict:
    part_keys = jax.random.split(jax.random.fold_in(jax.random.key(seed), part), 4)
    shared_keys = jax.random.split(jax.random.key(seed + 1), 8)
    mix_coef = normal_draw(part_keys[0], (MSA_ROWS, LOW_RANK), 1.0)
    res_feat = normal_draw(part_keys[1], (LOW_RANK, N_RES, MSA_DIM), 1.0)
    msa_noise = normal_draw(part_keys[2], (MSA_ROWS, N_RES, MSA_DIM), 0.5)
    msa_f32 = jnp.einsum('sr,rnm->snm', mix_coef, res_feat) * LOW_RANK ** -0.5 + msa_noise
    z_f32 = normal_draw(part_keys[3], (N_RES, N_RES, PAIR_DIM), 1.0)
    return {
        'z_pair': z_f32.astype(jnp.bfloat16),
        'msa_feat': msa_f32.astype(jnp.bfloat16),
        'ln_scale': (1.0 + normal_draw(shared_keys[0], (MSA_DIM,), 0.5)).astype(jnp.bfloat16),
        'ln_offset': normal_draw(shared_keys[1], (MSA_DIM,), 0.5).astype(jnp.bfloat16),
        'w_a': normal_draw(shared_keys[2], (MSA_DIM, HID_DIM), MSA_DIM ** -0.5).astype(jnp.bfloat16),
        'b_a': normal_draw(shared_keys[3], (HID_DIM,), 0.5).astype(jnp.bfloat16),
        'w_b': normal_draw(shared_keys[4], (MSA_DIM, HID_DIM), MSA_DIM ** -0.5).astype(jnp.bfloat16),
        'b_b': normal_draw(shared_keys[5], (HID_DIM,), 0.5).astype(jnp.bfloat16),
        'w_out': normal_draw(shared_keys[6], (HID_DIM * HID_DIM, PAIR_DIM), (HID_DIM * HID_DIM) ** -0.5).astype(jnp.bfloat16),
        'b_out': normal_draw(shared_keys[7], (PAIR_DIM,), 0.5).astype(jnp.bfloat16),
    }


def layer_norm(msa_feat, ln_scale, ln_offset):
    msa_f32 = msa_feat.astype(jnp.float32)
    mean_val = jnp.mean(msa_f32, axis=-1, keepdims=True)
    centred = msa_f32 - mean_val
    var_val = jnp.mean(centred * centred, axis=-1, keepdims=True)
    normed = centred / jnp.sqrt(var_val + LN_EPS)
    return (normed * ln_scale.astype(jnp.float32) + ln_offset.astype(jnp.float32)).astype(jnp.bfloat16)


def project(msa_norm, weight, bias_vec):
    flat_rows = msa_norm.reshape(-1, msa_norm.shape[-1])
    out_f32 = jnp.dot(flat_rows, weight, preferred_element_type=jnp.float32) + bias_vec.astype(jnp.float32)
    return out_f32.astype(jnp.bfloat16).reshape(msa_norm.shape[0], msa_norm.shape[1], weight.shape[1])


def reference(z_pair, msa_feat, ln_scale, ln_offset, w_a, b_a, w_b, b_b, w_out, b_out):
    msa_norm = layer_norm(msa_feat, ln_scale, ln_offset)
    proj_a = project(msa_norm, w_a, b_a).astype(jnp.float32)
    proj_b = project(msa_norm, w_b, b_b).astype(jnp.float32)
    w_cube = w_out.astype(jnp.float32).reshape(HID_DIM, HID_DIM, PAIR_DIM)
    bias_out = b_out.astype(jnp.float32)
    inv_seq = 1.0 / MSA_ROWS

    def tile_fn(tile_idx):
        row_start = tile_idx * ROW_TILE
        a_tile = lax.dynamic_slice_in_dim(proj_a, row_start, ROW_TILE, axis=1)
        z_tile = lax.dynamic_slice_in_dim(z_pair, row_start, ROW_TILE, axis=0)
        outer_prod = jnp.einsum('sic,sjd->icjd', a_tile, proj_b) * inv_seq
        outer_prod = outer_prod.astype(jnp.bfloat16).astype(jnp.float32)
        update = jnp.einsum('icjd,cdz->ijz', outer_prod, w_cube) + bias_out
        return (z_tile.astype(jnp.float32) + update).astype(jnp.bfloat16)

    row_tiles = lax.map(tile_fn, jnp.arange(N_RES // ROW_TILE))
    return row_tiles.reshape(N_RES, N_RES, PAIR_DIM)
```

```python
import jax
import jax.numpy as jnp
from jax import lax
from jax.experimental import pallas as pl
from jax.experimental.pallas import tpu as pltpu
from jax.sharding import PartitionSpec as P

MESH = pl.DeviceIdType.MESH
F32, BF16 = jnp.float32, jnp.bfloat16
LN_EPS = 1e-5
S, NL, M, H, N, Z = 512, 32, 64, 32, 256, 128
J = 8
NG = NL // J
CR = H * J
KR = CR // 4
NT = (((1,), (1,)), ((), ()))
NN = (((1,), (0,)), ((), ()))


def dot(x, y, dims=NN):
    return lax.dot_general(x, y, dims, preferred_element_type=F32)


def onehot(rows, cols, fn):
    r = lax.broadcasted_iota(jnp.int32, (rows, cols), 0)
    c = lax.broadcasted_iota(jnp.int32, (rows, cols), 1)
    return jnp.where(fn(r) == c, 1.0, 0.0).astype(BF16)


def kernel(z_hbm, m_hbm, lns_ref, lno_ref, wa_ref, ba_ref, wb_ref, bb_ref, wo_hbm, bo_ref, out_ref,
           b_buf, a_t, a_v, m_buf, b_f32, lhs2, w_buf, w_f32, w_v, z_buf, par,
           in_sem, send_sem, recv_sem):
    me = lax.axis_index("dap")
    core = me % 2
    xbit = (me // 2) % 2
    pt = me + 1 - 2 * core
    flip = pt - me
    xn = me + 2 - 4 * xbit
    yn = (me + 4) % 8
    dg = (xn + 4) % 8

    barrier = pltpu.get_barrier_semaphore()
    for dev in (pt, xn, yn):
        pl.semaphore_signal(barrier, inc=1, device_id={"dap": dev}, device_id_type=MESH)

    def m_copy(g):
        return pltpu.make_async_copy(m_hbm.at[pl.ds(g * J, J)], m_buf.at[g], in_sem.at[g])

    w_copy = pltpu.make_async_copy(wo_hbm, w_buf, in_sem.at[NG])
    z_copy = pltpu.make_async_copy(z_hbm, z_buf, in_sem.at[NG + 1])
    for g in range(NG):
        m_copy(g).start()
    w_copy.start()
    z_copy.start()

    def rdma(slot, g, dev, k):
        return pltpu.make_async_remote_copy(
            src_ref=b_buf.at[slot, g], dst_ref=b_buf.at[slot, g], send_sem=send_sem.at[k, g],
            recv_sem=recv_sem.at[slot, g], device_id={"dap": dev}, device_id_type=MESH)

    def arrived(slot, g):
        rdma(slot, g, pt, 0).wait_recv()

    def column(row, width):
        return jnp.broadcast_to(row.astype(F32).reshape(1, width), (128, width)).astype(BF16)

    eye = onehot(M, M, lambda r: r)
    order = onehot(2 * H, 2 * H, lambda r: jnp.where(r < H, r, H + 4 * ((r - H) % 8) + (r - H) // 8))
    w_ab = dot(order, jnp.concatenate([wa_ref[...], wb_ref[...]], axis=0)).astype(BF16)
    par[0] = dot(eye, column(lns_ref[...], M), NT)
    par[1] = dot(eye, column(lno_ref[...], M), NT)
    bias = jnp.concatenate([column(ba_ref[...], H), column(bb_ref[...], H)], axis=1)
    par[2] = dot(order, bias, NT)

    def lanes(i):
        return jnp.concatenate([par[i]] * (S // 128), axis=1)

    def produce(g, _):
        m_copy(g).wait()
        for n in range(J):
            x = m_buf[g, n].astype(F32)
            mean = jnp.sum(x, axis=0, keepdims=True) * (1.0 / M)
            x = x - mean
            var = jnp.sum(x * x, axis=0, keepdims=True) * (1.0 / M)
            x = x * lax.rsqrt(var + LN_EPS)
            x = (x * lanes(0) + lanes(1)).astype(BF16)
            r = dot(w_ab, x) + lanes(2)
            a_t[pl.ds(pl.multiple_of((g * J + n) * H, H), H), :] = r[:H].astype(BF16)
            for q in range(S // 128):
                b_f32[q, pl.ds(n, H, stride=J), :] = r[H:, 128 * q:128 * q + 128]
        b_buf[me, g] = jnp.concatenate([b_f32[q] for q in range(S // 128)], axis=1).astype(BF16)

        @pl.when(g == 0)
        def _():
            pl.semaphore_wait(barrier, 3)

        rdma(me, g, xn, 0).start()
        rdma(me, g, yn, 1).start()
        rdma(me, g, pt, 2).start()
        return 0

    lax.fori_loop(0, NG, produce, 0)

    eye256 = onehot(256, 256, lambda r: r)
    for t in range(4):
        for k in range(4):
            rows = jnp.concatenate(
                [a_t[pl.ds((8 * t + 4 * gg + (m + k) % 4) * H, H), :] for gg in range(2) for m in range(4)], axis=0)
            for h in range(S // 256):
                a_v[k, 256 * h:256 * h + 256, 256 * t:256 * t + 256] = dot(
                    eye256, rows[:, 256 * h:256 * h + 256], NT).astype(BF16)

    w_copy.wait()
    w_f32[...] = w_buf[...].astype(F32)
    for d in range(H):
        block = w_f32[pl.ds(d, H, stride=H), :].astype(BF16)
        for v in range(4):
            w_v[v, pl.ds((d // 4) * 128 + ((v - d) % 4) * H, H), :] = block
    z_copy.wait()

    bias_out = bo_ref[...].astype(F32).reshape(1, Z)
    lane = lax.broadcasted_iota(jnp.int32, (2 * KR, 128), 1) // H
    even = lane % 2 == 0
    outer = (lane == 0) | (lane == 3)
    low = lane < 2

    def unit(slot_a, g_a, slot_b, g_b):
        lhs = [jnp.concatenate([b_buf[slot_a, g_a, KR * k:KR * k + KR, :],
                                b_buf[slot_b, g_b, KR * k:KR * k + KR, :]], axis=0) for k in range(4)]
        for t in range(4):
            o = [dot(lhs[k], a_v[k, :, 256 * t:256 * t + 256]) * (1.0 / S) for k in range(4)]
            q = [[None, None] for _ in range(4)]
            for gg in range(2):
                p = [x[:, 128 * gg:128 * gg + 128] for x in o]
                e0, f0 = jnp.where(even, p[0], p[1]), jnp.where(even, p[2], p[3])
                e1, f1 = jnp.where(even, p[1], p[0]), jnp.where(even, p[3], p[2])
                q[0][gg] = jnp.where(outer, e0, f0)
                q[2][gg] = jnp.where(outer, f0, e0)
                q[1][gg] = jnp.where(low, e1, f1)
                q[3][gg] = jnp.where(low, f1, e1)
            for v in range(4):
                for c in range(2):
                    for e in range(8):
                        r0 = c * KR + e * J
                        lhs2[v, c * KR + 16 * t:c * KR + 16 * t + 16, 128 * e:128 * e + 128] = jnp.concatenate(
                            [q[v][0][r0:r0 + J], q[v][1][r0:r0 + J]], axis=0).astype(BF16)
        jc = (slot_a * NG + g_a, slot_b * NG + g_b)
        for v in range(4):
            u = dot(lhs2[v], w_v[v]) + bias_out
            for c in range(2):
                for G in range(8):
                    i = 4 * G + v
                    r0 = c * KR + G * J
                    out_ref[i, jc[c]] = (z_buf[i, jc[c]].astype(F32) + u[r0:r0 + J]).astype(BF16)

    def local(s, _):
        slot = me + flip * (s // 2)
        g = 2 * (s % 2)

        @pl.when(s >= 2)
        def _():
            arrived(slot, g)
            arrived(slot, g + 1)

        unit(slot, g, slot, g + 1)
        return 0

    lax.fori_loop(0, 4, local, 0)

    def near(s, _):
        g = s // 2
        p = s % 2
        sx, sy = xn + flip * p, yn + flip * p
        arrived(sx, g)
        arrived(sy, g)

        @pl.when(p == 0)
        def _():
            @pl.when(g % 2 == 0)
            def _():
                rdma(yn, g, xn, 3).start()

            @pl.when(g % 2 == 1)
            def _():
                rdma(xn, g, yn, 3).start()

            rdma(xn, g, pt, 4).start()
            rdma(yn, g, pt, 5).start()

        unit(sx, g, sy, g)
        return 0

    lax.fori_loop(0, 2 * NG, near, 0)

    def far(s, _):
        g = 2 * (s // 2)
        p = s % 2
        slot = dg + flip * p
        arrived(slot, g)
        arrived(slot, g + 1)

        @pl.when(p == 0)
        def _():
            rdma(dg, g, pt, 6).start()
            rdma(dg, g + 1, pt, 6).start()

        unit(slot, g, slot, g + 1)
        return 0

    lax.fori_loop(0, NG, far, 0)

    for k in range(7):
        for g in range(NG):
            rdma(me, g, pt, k).wait_send()


def local_update(z, m, lns, lno, wa, ba, wb, bb, wo, bo):
    hbm = pl.BlockSpec(memory_space=pltpu.HBM)
    vmem = pl.BlockSpec(memory_space=pltpu.VMEM)
    out = pl.pallas_call(
        kernel,
        out_shape=jax.ShapeDtypeStruct((NL, N // J, J, Z), BF16),
        in_specs=[hbm, hbm, vmem, vmem, vmem, vmem, vmem, vmem, hbm, vmem],
        out_specs=vmem,
        scratch_shapes=[
            pltpu.VMEM((8, NG, CR, S), BF16),
            pltpu.VMEM((NL * H, S), BF16),
            pltpu.VMEM((4, S, NL * H), BF16),
            pltpu.VMEM((NG, J, M, S), BF16),
            pltpu.VMEM((S // 128, CR, 128), F32),
            pltpu.VMEM((4, 2 * KR, H * H), BF16),
            pltpu.VMEM((H * H, Z), BF16),
            pltpu.VMEM((H * H, Z), F32),
            pltpu.VMEM((4, H * H, Z), BF16),
            pltpu.VMEM((NL, N // J, J, Z), BF16),
            pltpu.VMEM((3, M, 128), F32),
            pltpu.SemaphoreType.DMA((NG + 2,)),
            pltpu.SemaphoreType.DMA((7, NG)),
            pltpu.SemaphoreType.DMA((8, NG)),
        ],
        compiler_params=pltpu.CompilerParams(
            collective_id=0, has_side_effects=True, vmem_limit_bytes=48 * 1024 * 1024),
    )(z.reshape(NL, N // J, J, Z), m.transpose(1, 2, 0), lns.reshape(1, M), lno.reshape(1, M),
      wa.T, ba.reshape(1, H), wb.T, bb.reshape(1, H), wo, bo.reshape(1, Z))
    return out.reshape(NL, N, Z)


def solution(mesh):
    row, col, rep = P(("batch", "dap")), P(None, ("batch", "dap")), P()
    return jax.shard_map(local_update, mesh=mesh, in_specs=(row, col) + (rep,) * 8, out_specs=row, check_vma=False)
```

```python
import jax
import jax.numpy as jnp
from jax import lax
from jax.experimental import pallas as pl
from jax.experimental.pallas import tpu as pltpu
from jax.sharding import PartitionSpec as P

MESH = pl.DeviceIdType.MESH
F32, BF16 = jnp.float32, jnp.bfloat16
LN_EPS = 1e-5
S, NL, M, H, N, Z = 512, 32, 64, 32, 256, 128
J = 8
NG = NL // J
CR = H * J
KR = CR // 4
NT = (((1,), (1,)), ((), ()))
NN = (((1,), (0,)), ((), ()))


def dot(x, y, dims=NN):
    return lax.dot_general(x, y, dims, preferred_element_type=F32)


def onehot(rows, cols, fn):
    r = lax.broadcasted_iota(jnp.int32, (rows, cols), 0)
    c = lax.broadcasted_iota(jnp.int32, (rows, cols), 1)
    return jnp.where(fn(r) == c, 1.0, 0.0).astype(BF16)


def kernel(z_hbm, m_hbm, lns_hbm, lno_hbm, wa_hbm, ba_hbm, wb_hbm, bb_hbm, wo_hbm, bo_hbm, out_ref,
           b_buf, a_t, a_v, m_buf, b_f32, lhs2, w_buf, w_f32, w_v, z_buf, par,
           lns_ref, lno_ref, wa_ref, ba_ref, wb_ref, bb_ref, bo_ref,
           in_sem, send_sem, recv_sem):
    me = lax.axis_index("dap")
    core = me % 2
    xbit = (me // 2) % 2
    pt = me + 1 - 2 * core
    flip = pt - me
    xn = me + 2 - 4 * xbit
    yn = (me + 4) % 8
    dg = (xn + 4) % 8

    barrier = pltpu.get_barrier_semaphore()
    for dev in (pt, xn, yn):
        pl.semaphore_signal(barrier, inc=1, device_id={"dap": dev}, device_id_type=MESH)

    def m_copy(g):
        return pltpu.make_async_copy(m_hbm.at[pl.ds(g * J, J)], m_buf.at[g], in_sem.at[g])

    w_copy = pltpu.make_async_copy(wo_hbm, w_buf, in_sem.at[NG])
    z_copy = pltpu.make_async_copy(z_hbm, z_buf, in_sem.at[NG + 1])
    small = [pltpu.make_async_copy(src, dst, in_sem.at[NG + 2 + i]) for i, (src, dst) in enumerate((
        (lns_hbm, lns_ref), (lno_hbm, lno_ref), (wa_hbm, wa_ref), (ba_hbm, ba_ref),
        (wb_hbm, wb_ref), (bb_hbm, bb_ref), (bo_hbm, bo_ref)))]
    m_copy(0).start()
    for copy in small:
        copy.start()
    for g in range(1, NG):
        m_copy(g).start()
    w_copy.start()
    z_copy.start()

    def rdma(slot, g, dev, k):
        return pltpu.make_async_remote_copy(
            src_ref=b_buf.at[slot, g], dst_ref=b_buf.at[slot, g], send_sem=send_sem.at[k, g],
            recv_sem=recv_sem.at[slot, g], device_id={"dap": dev}, device_id_type=MESH)

    def arrived(slot, g):
        rdma(slot, g, pt, 0).wait_recv()

    for copy in small:
        copy.wait()

    def column(row, width):
        return jnp.broadcast_to(row.astype(F32).reshape(1, width), (128, width)).astype(BF16)

    eye = onehot(M, M, lambda r: r)
    order = onehot(2 * H, 2 * H, lambda r: jnp.where(r < H, r, H + 4 * ((r - H) % 8) + (r - H) // 8))
    w_ab = dot(order, jnp.concatenate([wa_ref[...], wb_ref[...]], axis=0)).astype(BF16)
    par[0] = dot(eye, column(lns_ref[...], M), NT)
    par[1] = dot(eye, column(lno_ref[...], M), NT)
    bias = jnp.concatenate([column(ba_ref[...], H), column(bb_ref[...], H)], axis=1)
    par[2] = dot(order, bias, NT)

    def lanes(i):
        return jnp.concatenate([par[i]] * (S // 128), axis=1)

    def produce(g, _):
        m_copy(g).wait()
        for n in range(J):
            x = m_buf[g, n].astype(F32)
            mean = jnp.sum(x, axis=0, keepdims=True) * (1.0 / M)
            x = x - mean
            var = jnp.sum(x * x, axis=0, keepdims=True) * (1.0 / M)
            x = x * lax.rsqrt(var + LN_EPS)
            x = (x * lanes(0) + lanes(1)).astype(BF16)
            r = dot(w_ab, x) + lanes(2)
            a_t[pl.ds(pl.multiple_of((g * J + n) * H, H), H), :] = r[:H].astype(BF16)
            for q in range(S // 128):
                b_f32[q, pl.ds(n, H, stride=J), :] = r[H:, 128 * q:128 * q + 128]
        b_buf[me, g] = jnp.concatenate([b_f32[q] for q in range(S // 128)], axis=1).astype(BF16)

        @pl.when(g == 0)
        def _():
            pl.semaphore_wait(barrier, 3)

        rdma(me, g, xn, 0).start()
        rdma(me, g, yn, 1).start()
        rdma(me, g, pt, 2).start()
        return 0

    lax.fori_loop(0, NG, produce, 0)

    eye256 = onehot(256, 256, lambda r: r)
    for t in range(4):
        for k in range(4):
            rows = jnp.concatenate(
                [a_t[pl.ds((8 * t + 4 * gg + (m + k) % 4) * H, H), :] for gg in range(2) for m in range(4)], axis=0)
            for h in range(S // 256):
                a_v[k, 256 * h:256 * h + 256, 256 * t:256 * t + 256] = dot(
                    eye256, rows[:, 256 * h:256 * h + 256], NT).astype(BF16)

    w_copy.wait()
    w_f32[...] = w_buf[...].astype(F32)
    for d in range(H):
        block = w_f32[pl.ds(d, H, stride=H), :].astype(BF16)
        for v in range(4):
            w_v[v, pl.ds((d // 4) * 128 + ((v - d) % 4) * H, H), :] = block
    z_copy.wait()

    bias_out = bo_ref[...].astype(F32).reshape(1, Z)
    lane = lax.broadcasted_iota(jnp.int32, (2 * KR, 128), 1) // H
    even = lane % 2 == 0
    outer = (lane == 0) | (lane == 3)
    low = lane < 2

    def unit(slot_a, g_a, slot_b, g_b):
        lhs = [jnp.concatenate([b_buf[slot_a, g_a, KR * k:KR * k + KR, :],
                                b_buf[slot_b, g_b, KR * k:KR * k + KR, :]], axis=0) for k in range(4)]
        for t in range(4):
            o = [dot(lhs[k], a_v[k, :, 256 * t:256 * t + 256]) * (1.0 / S) for k in range(4)]
            q = [[None, None] for _ in range(4)]
            for gg in range(2):
                p = [x[:, 128 * gg:128 * gg + 128] for x in o]
                e0, f0 = jnp.where(even, p[0], p[1]), jnp.where(even, p[2], p[3])
                e1, f1 = jnp.where(even, p[1], p[0]), jnp.where(even, p[3], p[2])
                q[0][gg] = jnp.where(outer, e0, f0)
                q[2][gg] = jnp.where(outer, f0, e0)
                q[1][gg] = jnp.where(low, e1, f1)
                q[3][gg] = jnp.where(low, f1, e1)
            for v in range(4):
                for c in range(2):
                    for e in range(8):
                        r0 = c * KR + e * J
                        lhs2[v, c * KR + 16 * t:c * KR + 16 * t + 16, 128 * e:128 * e + 128] = jnp.concatenate(
                            [q[v][0][r0:r0 + J], q[v][1][r0:r0 + J]], axis=0).astype(BF16)
        jc = (slot_a * NG + g_a, slot_b * NG + g_b)
        for v in range(4):
            u = dot(lhs2[v], w_v[v]) + bias_out
            for c in range(2):
                for G in range(8):
                    i = 4 * G + v
                    r0 = c * KR + G * J
                    out_ref[i, jc[c]] = (z_buf[i, jc[c]].astype(F32) + u[r0:r0 + J]).astype(BF16)

    def local(s, _):
        slot = me + flip * (s // 2)
        g = 2 * (s % 2)

        @pl.when(s >= 2)
        def _():
            arrived(slot, g)
            arrived(slot, g + 1)

        unit(slot, g, slot, g + 1)
        return 0

    lax.fori_loop(0, 4, local, 0)

    def near(s, _):
        g = s // 2
        p = s % 2
        sx, sy = xn + flip * p, yn + flip * p
        arrived(sx, g)
        arrived(sy, g)

        @pl.when(p == 0)
        def _():
            @pl.when(g % 2 == 0)
            def _():
                rdma(yn, g, xn, 3).start()

            @pl.when(g % 2 == 1)
            def _():
                rdma(xn, g, yn, 3).start()

            rdma(xn, g, pt, 4).start()
            rdma(yn, g, pt, 5).start()

        unit(sx, g, sy, g)
        return 0

    lax.fori_loop(0, 2 * NG, near, 0)

    def far(s, _):
        g = 2 * (s // 2)
        p = s % 2
        slot = dg + flip * p
        arrived(slot, g)
        arrived(slot, g + 1)

        @pl.when(p == 0)
        def _():
            rdma(dg, g, pt, 6).start()
            rdma(dg, g + 1, pt, 6).start()

        unit(slot, g, slot, g + 1)
        return 0

    lax.fori_loop(0, NG, far, 0)

    for k in range(7):
        for g in range(NG):
            rdma(me, g, pt, k).wait_send()


def local_update(z, m, lns, lno, wa, ba, wb, bb, wo, bo):
    hbm = pl.BlockSpec(memory_space=pltpu.HBM)
    vmem = pl.BlockSpec(memory_space=pltpu.VMEM)
    args = (z.reshape(NL, N // J, J, Z), m.transpose(1, 2, 0), lns.reshape(1, M), lno.reshape(1, M),
            wa.T, ba.reshape(1, H), wb.T, bb.reshape(1, H), wo, bo.reshape(1, Z))
    out = pl.pallas_call(
        kernel,
        out_shape=jax.ShapeDtypeStruct((NL, N // J, J, Z), BF16),
        in_specs=[hbm] * len(args),
        out_specs=vmem,
        scratch_shapes=[
            pltpu.VMEM((8, NG, CR, S), BF16),
            pltpu.VMEM((NL * H, S), BF16),
            pltpu.VMEM((4, S, NL * H), BF16),
            pltpu.VMEM((NG, J, M, S), BF16),
            pltpu.VMEM((S // 128, CR, 128), F32),
            pltpu.VMEM((4, 2 * KR, H * H), BF16),
            pltpu.VMEM((H * H, Z), BF16),
            pltpu.VMEM((H * H, Z), F32),
            pltpu.VMEM((4, H * H, Z), BF16),
            pltpu.VMEM((NL, N // J, J, Z), BF16),
            pltpu.VMEM((3, M, 128), F32),
            pltpu.VMEM((1, M), BF16),
            pltpu.VMEM((1, M), BF16),
            pltpu.VMEM((H, M), BF16),
            pltpu.VMEM((1, H), BF16),
            pltpu.VMEM((H, M), BF16),
            pltpu.VMEM((1, H), BF16),
            pltpu.VMEM((1, Z), BF16),
            pltpu.SemaphoreType.DMA((NG + 9,)),
            pltpu.SemaphoreType.DMA((7, NG)),
            pltpu.SemaphoreType.DMA((8, NG)),
        ],
        compiler_params=pltpu.CompilerParams(
            collective_id=0, has_side_effects=True, vmem_limit_bytes=48 * 1024 * 1024),
    )(*(pltpu.with_memory_space_constraint(x, pltpu.HBM) for x in args))
    return out.reshape(NL, N, Z)


def solution(mesh):
    row, col, rep = P(("batch", "dap")), P(None, ("batch", "dap")), P()
    return jax.shard_map(local_update, mesh=mesh, in_specs=(row, col) + (rep,) * 8, out_specs=row, check_vma=False)
```

```python
import jax
import jax.numpy as jnp
from jax import lax
from jax.experimental import pallas as pl
from jax.experimental.pallas import tpu as pltpu
from jax.sharding import PartitionSpec as P

MESH = pl.DeviceIdType.MESH
F32, BF16 = jnp.float32, jnp.bfloat16
LN_EPS = 1e-5
S, NL, M, H, N, Z = 512, 32, 64, 32, 256, 128
J = 8
NG = NL // J
CR = H * J
KR = CR // 4
HS = S // 2
NT = (((1,), (1,)), ((), ()))
NN = (((1,), (0,)), ((), ()))


def dot(x, y, dims=NN):
    return lax.dot_general(x, y, dims, preferred_element_type=F32)


def onehot(rows, cols, fn):
    r = lax.broadcasted_iota(jnp.int32, (rows, cols), 0)
    c = lax.broadcasted_iota(jnp.int32, (rows, cols), 1)
    return jnp.where(fn(r) == c, 1.0, 0.0).astype(BF16)


def kernel(z_hbm, m_hbm, lns_hbm, lno_hbm, wa_hbm, ba_hbm, wb_hbm, bb_hbm, wo_hbm, bo_hbm, out_ref,
           b_buf, a_t, a_v, m_buf, b_f32, lhs2, w_buf, w_f32, w_v, z_buf, par,
           lns_ref, lno_ref, wa_ref, ba_ref, wb_ref, bb_ref, bo_ref,
           part, in_sem, send_sem, recv_sem):
    me = lax.axis_index("dap")
    core = me % 2
    xbit = (me // 2) % 2
    pt = me + 1 - 2 * core
    flip = pt - me
    xn = me + 2 - 4 * xbit
    yn = (me + 4) % 8
    dg = (xn + 4) % 8

    barrier = pltpu.get_barrier_semaphore()
    for dev in (pt, xn, yn):
        pl.semaphore_signal(barrier, inc=1, device_id={"dap": dev}, device_id_type=MESH)

    def m_half(h):
        return pltpu.make_async_copy(
            m_hbm.at[pl.ds(0, J), :, pl.ds(h * HS, HS)], m_buf.at[pl.ds(0, J), :, pl.ds(h * HS, HS)], in_sem.at[h])

    m_rest = pltpu.make_async_copy(m_hbm.at[pl.ds(J, NL - J)], m_buf.at[pl.ds(J, NL - J)], in_sem.at[2])
    w_copy = pltpu.make_async_copy(wo_hbm, w_buf, in_sem.at[3])
    z_copy = pltpu.make_async_copy(z_hbm, z_buf, in_sem.at[4])
    small = [pltpu.make_async_copy(src, dst, in_sem.at[5 + i]) for i, (src, dst) in enumerate((
        (lns_hbm, lns_ref), (lno_hbm, lno_ref), (wa_hbm, wa_ref), (ba_hbm, ba_ref),
        (wb_hbm, wb_ref), (bb_hbm, bb_ref), (bo_hbm, bo_ref)))]
    m_half(0).start()
    for copy in small:
        copy.start()
    m_half(1).start()
    m_rest.start()
    w_copy.start()
    z_copy.start()

    def whole(slot, g, dev, sem):
        return pltpu.make_async_remote_copy(
            src_ref=b_buf.at[slot, g], dst_ref=b_buf.at[slot, g], send_sem=send_sem.at[0],
            recv_sem=recv_sem.at[sem], device_id={"dap": dev}, device_id_type=MESH)

    def half(slot, g, h, dev, sem, k=1):
        return pltpu.make_async_remote_copy(
            src_ref=b_buf.at[slot, g, h], dst_ref=b_buf.at[slot, g, h], send_sem=send_sem.at[k],
            recv_sem=recv_sem.at[sem], device_id={"dap": dev}, device_id_type=MESH)

    def span(ref, k, sem):
        return pltpu.make_async_remote_copy(
            src_ref=ref, dst_ref=ref, send_sem=send_sem.at[k], recv_sem=recv_sem.at[sem],
            device_id={"dap": pt}, device_id_type=MESH)

    def arrived(sem):
        span(b_buf.at[0, pl.ds(0, 2)], 0, sem).wait_recv()

    def arrived_halves(sem):
        span(b_buf.at[0, 0], 0, sem).wait_recv()

    for copy in small:
        copy.wait()

    def column(row, width):
        return jnp.broadcast_to(row.astype(F32).reshape(1, width), (128, width)).astype(BF16)

    eye = onehot(M, M, lambda r: r)
    order = onehot(2 * H, 2 * H, lambda r: jnp.where(r < H, r, H + 4 * ((r - H) % 8) + (r - H) // 8))
    w_ab = dot(order, jnp.concatenate([wa_ref[...], wb_ref[...]], axis=0)).astype(BF16)
    par[0] = dot(eye, column(lns_ref[...], M), NT)
    par[1] = dot(eye, column(lno_ref[...], M), NT)
    bias = jnp.concatenate([column(ba_ref[...], H), column(bb_ref[...], H)], axis=1)
    par[2] = dot(order, bias, NT)

    def lanes(i):
        return jnp.concatenate([par[i]] * (HS // 128), axis=1)

    def produce(g, _):
        for h in range(2):
            @pl.when(g == 0)
            def _():
                m_half(h).wait()

            if h == 0:
                @pl.when(g == 1)
                def _():
                    m_rest.wait()

            for n in range(J):
                x = m_buf[g * J + n, :, HS * h:HS * h + HS].astype(F32)
                mean = jnp.sum(x, axis=0, keepdims=True) * (1.0 / M)
                x = x - mean
                var = jnp.sum(x * x, axis=0, keepdims=True) * (1.0 / M)
                x = x * lax.rsqrt(var + LN_EPS)
                x = (x * lanes(0) + lanes(1)).astype(BF16)
                r = dot(w_ab, x) + lanes(2)
                a_t[pl.ds(pl.multiple_of((g * J + n) * H, H), H), HS * h:HS * h + HS] = r[:H].astype(BF16)
                for q in range(HS // 128):
                    b_f32[q, pl.ds(n, H, stride=J), :] = r[H:, 128 * q:128 * q + 128]
            b_buf[me, g, h] = jnp.concatenate([b_f32[q] for q in range(HS // 128)], axis=1).astype(BF16)

            @pl.when(g == 0)
            def _():
                if h == 0:
                    pl.semaphore_wait(barrier, 3)
                half(me, g, h, xn, 2, 0).start()
                half(me, g, h, yn, 2, 0).start()
                half(me, g, h, pt, 0, 0).start()

        @pl.when(g > 0)
        def _():
            whole(me, g, xn, 2 + g).start()
            whole(me, g, yn, 2 + g).start()
            whole(me, g, pt, g // 2).start()

        return 0

    lax.fori_loop(0, NG, produce, 0)

    eye256 = onehot(256, 256, lambda r: r)
    for t in range(4):
        for k in range(4):
            rows = jnp.concatenate(
                [a_t[pl.ds((8 * t + 4 * gg + (m + k) % 4) * H, H), :] for gg in range(2) for m in range(4)], axis=0)
            for h in range(S // 256):
                a_v[k, 256 * h:256 * h + 256, 256 * t:256 * t + 256] = dot(
                    eye256, rows[:, 256 * h:256 * h + 256], NT).astype(BF16)

    w_copy.wait()
    w_f32[...] = w_buf[...].astype(F32)
    for d in range(H):
        block = w_f32[pl.ds(d, H, stride=H), :].astype(BF16)
        for v in range(4):
            w_v[v, pl.ds((d // 4) * 128 + ((v - d) % 4) * H, H), :] = block
    z_copy.wait()

    bias_out = bo_ref[...].astype(F32).reshape(1, Z)
    lane = lax.broadcasted_iota(jnp.int32, (2 * KR, 128), 1) // H
    even = lane % 2 == 0
    ends = (lane == 0) | (lane == 3)
    low = lane < 2

    def pair(slot_a, g_a, slot_b, g_b, k, h):
        return jnp.concatenate([b_buf[slot_a, g_a, h, KR * k:KR * k + KR, :],
                                b_buf[slot_b, g_b, h, KR * k:KR * k + KR, :]], axis=0)

    def outer(k, h, t, chunks):
        return dot(pair(*chunks, k, h), a_v[k, HS * h:HS * h + HS, 256 * t:256 * t + 256])

    def finish(chunks, product):
        for t in range(4):
            o = [product(k, t) * (1.0 / S) for k in range(4)]
            q = [[None, None] for _ in range(4)]
            for gg in range(2):
                p = [x[:, 128 * gg:128 * gg + 128] for x in o]
                e0, f0 = jnp.where(even, p[0], p[1]), jnp.where(even, p[2], p[3])
                e1, f1 = jnp.where(even, p[1], p[0]), jnp.where(even, p[3], p[2])
                q[0][gg] = jnp.where(ends, e0, f0)
                q[2][gg] = jnp.where(ends, f0, e0)
                q[1][gg] = jnp.where(low, e1, f1)
                q[3][gg] = jnp.where(low, f1, e1)
            for v in range(4):
                for c in range(2):
                    for e in range(8):
                        r0 = c * KR + e * J
                        lhs2[v, c * KR + 16 * t:c * KR + 16 * t + 16, 128 * e:128 * e + 128] = jnp.concatenate(
                            [q[v][0][r0:r0 + J], q[v][1][r0:r0 + J]], axis=0).astype(BF16)
        slot_a, g_a, slot_b, g_b = chunks
        jc = (slot_a * NG + g_a, slot_b * NG + g_b)
        for v in range(4):
            u = dot(lhs2[v], w_v[v]) + bias_out
            for c in range(2):
                for G in range(8):
                    i = 4 * G + v
                    r0 = c * KR + G * J
                    out_ref[i, jc[c]] = (z_buf[i, jc[c]].astype(F32) + u[r0:r0 + J]).astype(BF16)

    def unit(*chunks):
        lhs = [jnp.concatenate([pair(*chunks, k, h) for h in range(2)], axis=1) for k in range(4)]
        finish(chunks, lambda k, t: dot(lhs[k], a_v[k, :, 256 * t:256 * t + 256]))

    def local(s, _):
        slot = me + flip * (s // 2)
        g = 2 * (s % 2)

        @pl.when(s >= 2)
        def _():
            arrived(s % 2)

        unit(slot, g, slot, g + 1)
        return 0

    lax.fori_loop(0, 4, local, 0)

    def near(s, _):
        g = s // 2
        p = s % 2

        @pl.when(p == 0)
        def _():
            arrived(2 + g)
            for gc in range(NG):
                @pl.when(g == gc)
                def _():
                    slot, dev = (yn, xn) if gc % 2 == 0 else (xn, yn)
                    if gc < 2:
                        whole(slot, gc, dev, 10).start()
                    else:
                        @pl.when(core == 1)
                        def _():
                            half(slot, gc, 0, dev, 12).start()
                            half(slot, gc, 1, dev, 13).start()

                        @pl.when(core == 0)
                        def _():
                            half(slot, gc, 0, dev, 14).start()

            whole(xn, g, pt, 6 + g).start()
            whole(yn, g, pt, 6 + g).start()

        @pl.when(p == 1)
        def _():
            arrived(6 + g)

            @pl.when(core == 1)
            def _():
                @pl.when(g == 2)
                def _():
                    half(yn + flip, 2, 1, xn, 15).start()

                @pl.when(g == 3)
                def _():
                    half(xn + flip, 3, 1, yn, 15).start()

        unit(xn + flip * p, g, yn + flip * p, g)
        return 0

    lax.fori_loop(0, 2 * NG, near, 0)

    d1 = dg - core + 1
    d0 = dg - core

    def hand_on(slot, h, sem):
        half(slot, 2, h, pt, sem).start()
        half(slot, 3, h, pt, sem).start()

    def first_half(slot):
        for t in range(4):
            for k in range(4):
                part[slot % 2, k, :, 256 * t:256 * t + 256] = outer(k, 0, t, (slot, 2, slot, 3))

    def second_half(slot):
        chunks = (slot, 2, slot, 3)
        finish(chunks, lambda k, t: part[slot % 2, k, :, 256 * t:256 * t + 256] + outer(k, 1, t, chunks))

    def far_from():
        arrived(10)
        whole(dg, 0, pt, 11).start()
        whole(dg, 1, pt, 11).start()

    @pl.when(core == 1)
    def _():
        def far(q, _):
            @pl.when(q == 0)
            def _():
                far_from()

            @pl.when(q == 1)
            def _():
                arrived_halves(12)
                hand_on(d1, 0, 12)
                first_half(d1)
                arrived_halves(13)
                hand_on(d1, 1, 13)
                arrived(11)

            @pl.when(q == 2)
            def _():
                arrived_halves(15)
                hand_on(d0, 1, 15)
                second_half(d1)
                arrived_halves(14)

            slot = d1 - (q + 1) // 2
            g = 2 * (q // 2)
            unit(slot, g, slot, g + 1)
            return 0

        lax.fori_loop(0, 3, far, 0)

    @pl.when(core == 0)
    def _():
        def far(q, _):
            @pl.when(q == 0)
            def _():
                far_from()

            @pl.when(q == 1)
            def _():
                arrived(11)

            unit(d0 + q, 0, d0 + q, 1)
            return 0

        lax.fori_loop(0, 2, far, 0)

        def first(q, _):
            arrived_halves(12 + 2 * q)

            @pl.when(q == 1)
            def _():
                hand_on(d0, 0, 14)

            first_half(d1 - q)
            return 0

        lax.fori_loop(0, 2, first, 0)

        def second(q, _):
            arrived_halves(13 + 2 * q)
            second_half(d1 - q)
            return 0

        lax.fori_loop(0, 2, second, 0)

    span(b_buf.at[pl.ds(0, 6)], 0, 0).wait_send()

    @pl.when(core == 1)
    def _():
        span(b_buf.at[pl.ds(0, 2), pl.ds(0, 3)], 1, 0).wait_send()

    @pl.when(core == 0)
    def _():
        span(b_buf.at[0, pl.ds(0, 2)], 1, 0).wait_send()


def local_update(z, m, lns, lno, wa, ba, wb, bb, wo, bo):
    hbm = pl.BlockSpec(memory_space=pltpu.HBM)
    vmem = pl.BlockSpec(memory_space=pltpu.VMEM)
    args = (z.reshape(NL, N // J, J, Z), m.transpose(1, 2, 0), lns.reshape(1, M), lno.reshape(1, M),
            wa.T, ba.reshape(1, H), wb.T, bb.reshape(1, H), wo, bo.reshape(1, Z))
    out = pl.pallas_call(
        kernel,
        out_shape=jax.ShapeDtypeStruct((NL, N // J, J, Z), BF16),
        in_specs=[hbm] * len(args),
        out_specs=vmem,
        scratch_shapes=[
            pltpu.VMEM((8, NG, 2, CR, HS), BF16),
            pltpu.VMEM((NL * H, S), BF16),
            pltpu.VMEM((4, S, NL * H), BF16),
            pltpu.VMEM((NL, M, S), BF16),
            pltpu.VMEM((HS // 128, CR, 128), F32),
            pltpu.VMEM((4, 2 * KR, H * H), BF16),
            pltpu.VMEM((H * H, Z), BF16),
            pltpu.VMEM((H * H, Z), F32),
            pltpu.VMEM((4, H * H, Z), BF16),
            pltpu.VMEM((NL, N // J, J, Z), BF16),
            pltpu.VMEM((3, M, 128), F32),
            pltpu.VMEM((1, M), BF16),
            pltpu.VMEM((1, M), BF16),
            pltpu.VMEM((H, M), BF16),
            pltpu.VMEM((1, H), BF16),
            pltpu.VMEM((H, M), BF16),
            pltpu.VMEM((1, H), BF16),
            pltpu.VMEM((1, Z), BF16),
            pltpu.VMEM((2, 4, 2 * KR, NL * H), F32),
            pltpu.SemaphoreType.DMA((12,)),
            pltpu.SemaphoreType.DMA((2,)),
            pltpu.SemaphoreType.DMA((16,)),
        ],
        compiler_params=pltpu.CompilerParams(
            collective_id=0, has_side_effects=True, vmem_limit_bytes=48 * 1024 * 1024),
    )(*(pltpu.with_memory_space_constraint(x, pltpu.HBM) for x in args))
    return out.reshape(NL, N, Z)


def solution(mesh):
    row, col, rep = P(("batch", "dap")), P(None, ("batch", "dap")), P()
    return jax.shard_map(local_update, mesh=mesh, in_specs=(row, col) + (rep,) * 8, out_specs=row, check_vma=False)
```

```python
import jax
import jax.numpy as jnp
from jax import lax
from jax.experimental import pallas as pl
from jax.experimental.pallas import tpu as pltpu
from jax.sharding import PartitionSpec as P

MESH = pl.DeviceIdType.MESH
F32, BF16 = jnp.float32, jnp.bfloat16
LN_EPS = 1e-5
S, NL, M, H, N, Z = 512, 32, 64, 32, 256, 128
J = 8
NG = NL // J
CR = H * J
KR = CR // 4
HS = S // 2
HQ = HS // 128
NT = (((1,), (1,)), ((), ()))
NN = (((1,), (0,)), ((), ()))


def dot(x, y, dims=NN):
    return lax.dot_general(x, y, dims, preferred_element_type=F32)


def onehot(rows, cols, fn):
    r = lax.broadcasted_iota(jnp.int32, (rows, cols), 0)
    c = lax.broadcasted_iota(jnp.int32, (rows, cols), 1)
    return jnp.where(fn(r) == c, 1.0, 0.0).astype(BF16)


def kernel(z_hbm, m_hbm, lns_hbm, lno_hbm, wa_hbm, ba_hbm, wb_hbm, bb_hbm, wo_hbm, bo_hbm, out_ref,
           b_buf, a_t, a_v, m_buf, b_f32, lhs2, w_buf, w_f32, w_v, z_buf, par,
           lns_ref, lno_ref, wa_ref, ba_ref, wb_ref, bb_ref, bo_ref,
           part, in_sem, send_sem, recv_sem):
    me = lax.axis_index("dap")
    core = me % 2
    xbit = (me // 2) % 2
    pt = me + 1 - 2 * core
    flip = pt - me
    xn = me + 2 - 4 * xbit
    yn = (me + 4) % 8
    dg = (xn + 4) % 8

    barrier = pltpu.get_barrier_semaphore()
    for dev in (pt, xn, yn):
        pl.semaphore_signal(barrier, inc=1, device_id={"dap": dev}, device_id_type=MESH)

    def m_part(i):
        part_of = pl.ds(0, J), slice(None), pl.ds(i * 128, 128)
        return pltpu.make_async_copy(m_hbm.at[part_of], m_buf.at[part_of], in_sem.at[i])

    m_rest = pltpu.make_async_copy(m_hbm.at[pl.ds(J, NL - J)], m_buf.at[pl.ds(J, NL - J)], in_sem.at[12])
    w_copy = pltpu.make_async_copy(wo_hbm, w_buf, in_sem.at[13])
    z_copy = pltpu.make_async_copy(z_hbm, z_buf, in_sem.at[4])
    small = [pltpu.make_async_copy(src, dst, in_sem.at[5 + i]) for i, (src, dst) in enumerate((
        (lns_hbm, lns_ref), (lno_hbm, lno_ref), (wa_hbm, wa_ref), (ba_hbm, ba_ref),
        (wb_hbm, wb_ref), (bb_hbm, bb_ref), (bo_hbm, bo_ref)))]
    m_part(0).start()
    for copy in small:
        copy.start()
    for i in range(1, S // 128):
        m_part(i).start()
    m_rest.start()
    w_copy.start()
    z_copy.start()

    def whole(slot, g, dev, sem):
        return pltpu.make_async_remote_copy(
            src_ref=b_buf.at[slot, g], dst_ref=b_buf.at[slot, g], send_sem=send_sem.at[0],
            recv_sem=recv_sem.at[sem], device_id={"dap": dev}, device_id_type=MESH)

    def half(slot, g, h, dev, sem, k=1):
        return pltpu.make_async_remote_copy(
            src_ref=b_buf.at[slot, g, h], dst_ref=b_buf.at[slot, g, h], send_sem=send_sem.at[k],
            recv_sem=recv_sem.at[sem], device_id={"dap": dev}, device_id_type=MESH)

    def span(ref, k, sem):
        return pltpu.make_async_remote_copy(
            src_ref=ref, dst_ref=ref, send_sem=send_sem.at[k], recv_sem=recv_sem.at[sem],
            device_id={"dap": pt}, device_id_type=MESH)

    def arrived(sem):
        span(b_buf.at[0, pl.ds(0, 2)], 0, sem).wait_recv()

    def arrived_halves(sem):
        span(b_buf.at[0, 0], 0, sem).wait_recv()

    for copy in small:
        copy.wait()

    def column(row, width):
        return jnp.broadcast_to(row.astype(F32).reshape(1, width), (128, width)).astype(BF16)

    eye = onehot(M, M, lambda r: r)
    order = onehot(2 * H, 2 * H, lambda r: jnp.where(r < H, r, H + 4 * ((r - H) % 8) + (r - H) // 8))
    w_ab = dot(order, jnp.concatenate([wa_ref[...], wb_ref[...]], axis=0)).astype(BF16)
    par[0] = dot(eye, column(lns_ref[...], M), NT)
    par[1] = dot(eye, column(lno_ref[...], M), NT)
    bias = jnp.concatenate([column(ba_ref[...], H), column(bb_ref[...], H)], axis=1)
    par[2] = dot(order, bias, NT)

    def make(g, h, q0, nq):
        def lanes(i):
            return jnp.concatenate([par[i]] * nq, axis=1)

        lo = HS * h + 128 * q0
        for n in range(J):
            x = m_buf[g * J + n, :, lo:lo + 128 * nq].astype(F32)
            mean = jnp.sum(x, axis=0, keepdims=True) * (1.0 / M)
            x = x - mean
            var = jnp.sum(x * x, axis=0, keepdims=True) * (1.0 / M)
            x = x * lax.rsqrt(var + LN_EPS)
            x = (x * lanes(0) + lanes(1)).astype(BF16)
            r = dot(w_ab, x) + lanes(2)
            for q in range(nq):
                rq = r[:, 128 * q:128 * q + 128]
                a_t[h, q0 + q, pl.ds((g * J + n) * H, H), :] = rq[:H].astype(BF16)
                b_f32[q0 + q, pl.ds(n, H, stride=J), :] = rq[H:]
        for q in range(q0, q0 + nq):
            b_buf[me, g, h, q] = b_f32[q].astype(BF16)

    for i in range(S // 128):
        m_part(i).wait()
        h, q = i // HQ, i % HQ
        make(0, h, q, 1)
        if i == 0:
            pl.semaphore_wait(barrier, 3)
        for dev, sem in ((xn, 2), (yn, 2), (pt, 0)):
            piece = b_buf.at[me, 0, h, q]
            pltpu.make_async_remote_copy(
                src_ref=piece, dst_ref=piece, send_sem=send_sem.at[0], recv_sem=recv_sem.at[sem],
                device_id={"dap": dev}, device_id_type=MESH).start()
    m_rest.wait()

    def produce(g, _):
        for h in range(2):
            make(g, h, 0, HQ)
        whole(me, g, xn, 2 + g).start()
        whole(me, g, yn, 2 + g).start()
        whole(me, g, pt, g // 2).start()
        return 0

    lax.fori_loop(1, NG, produce, 0)

    eye256 = onehot(256, 256, lambda r: r)
    for t in range(4):
        for k in range(4):
            for h in range(2):
                rows = jnp.concatenate([jnp.concatenate(
                    [a_t[h, q, pl.ds((8 * t + 4 * gg + (m + k) % 4) * H, H), :] for gg in range(2) for m in range(4)],
                    axis=0) for q in range(HQ)], axis=1)
                block = dot(eye256, rows, NT).astype(BF16)
                for gg in range(2):
                    a_v[k, 2 * t + gg, HS * h:HS * h + HS, :] = block[:, 128 * gg:128 * gg + 128]

    w_copy.wait()
    w_f32[...] = w_buf[...].astype(F32)
    for d in range(H):
        block = w_f32[pl.ds(d, H, stride=H), :].astype(BF16)
        for v in range(4):
            w_v[v, pl.ds((d // 4) * 128 + ((v - d) % 4) * H, H), :] = block
    z_copy.wait()

    bias_out = bo_ref[...].astype(F32).reshape(1, Z)
    lane = lax.broadcasted_iota(jnp.int32, (2 * KR, 128), 1) // H
    even = lane % 2 == 0
    ends = (lane == 0) | (lane == 3)
    low = lane < 2

    def pair(slot_a, g_a, slot_b, g_b, k, h):
        return jnp.concatenate([jnp.concatenate(
            [b_buf[slot_a, g_a, h, q, KR * k:KR * k + KR, :], b_buf[slot_b, g_b, h, q, KR * k:KR * k + KR, :]],
            axis=0) for q in range(HQ)], axis=1)

    def a_cols(k, t, lo, n):
        return jnp.concatenate([a_v[k, 2 * t + gg, lo:lo + n, :] for gg in range(2)], axis=1)

    def outer(k, h, t, chunks):
        return dot(pair(*chunks, k, h), a_cols(k, t, HS * h, HS))

    def finish(chunks, product):
        for t in range(4):
            o = [product(k, t) * (1.0 / S) for k in range(4)]
            q = [[None, None] for _ in range(4)]
            for gg in range(2):
                p = [x[:, 128 * gg:128 * gg + 128] for x in o]
                e0, f0 = jnp.where(even, p[0], p[1]), jnp.where(even, p[2], p[3])
                e1, f1 = jnp.where(even, p[1], p[0]), jnp.where(even, p[3], p[2])
                q[0][gg] = jnp.where(ends, e0, f0)
                q[2][gg] = jnp.where(ends, f0, e0)
                q[1][gg] = jnp.where(low, e1, f1)
                q[3][gg] = jnp.where(low, f1, e1)
            for v in range(4):
                for c in range(2):
                    for e in range(8):
                        r0 = c * KR + e * J
                        lhs2[v, e, c * KR + 16 * t:c * KR + 16 * t + 16, :] = jnp.concatenate(
                            [q[v][0][r0:r0 + J], q[v][1][r0:r0 + J]], axis=0).astype(BF16)
        slot_a, g_a, slot_b, g_b = chunks
        jc = (slot_a * NG + g_a, slot_b * NG + g_b)
        for v in range(4):
            u = dot(jnp.concatenate([lhs2[v, e] for e in range(8)], axis=1),
                    jnp.concatenate([w_v[v], jnp.zeros((H * H, Z), BF16)], axis=1))[:, :Z] + bias_out
            for c in range(2):
                for G in range(8):
                    i = 4 * G + v
                    r0 = c * KR + G * J
                    out_ref[i, jc[c]] = (z_buf[i, jc[c]].astype(F32) + u[r0:r0 + J]).astype(BF16)

    def unit(*chunks):
        lhs = [jnp.concatenate([pair(*chunks, k, h) for h in range(2)], axis=1) for k in range(4)]
        finish(chunks, lambda k, t: dot(lhs[k], a_cols(k, t, 0, S)))

    def local(s, _):
        slot = me + flip * (s // 2)
        g = 2 * (s % 2)

        @pl.when(s >= 2)
        def _():
            arrived(s % 2)

        unit(slot, g, slot, g + 1)
        return 0

    lax.fori_loop(0, 4, local, 0)

    def near(s, _):
        g = s // 2
        p = s % 2

        @pl.when(p == 0)
        def _():
            arrived(2 + g)
            for gc in range(NG):
                @pl.when(g == gc)
                def _():
                    slot, dev = (yn, xn) if gc % 2 == 0 else (xn, yn)
                    if gc < 2:
                        whole(slot, gc, dev, 10).start()
                    else:
                        @pl.when(core == 1)
                        def _():
                            half(slot, gc, 0, dev, 12).start()
                            half(slot, gc, 1, dev, 13).start()

                        @pl.when(core == 0)
                        def _():
                            half(slot, gc, 0, dev, 14).start()

            whole(xn, g, pt, 6 + g).start()
            whole(yn, g, pt, 6 + g).start()

        @pl.when(p == 1)
        def _():
            arrived(6 + g)

            @pl.when(core == 1)
            def _():
                @pl.when(g == 2)
                def _():
                    half(yn + flip, 2, 1, xn, 15).start()

                @pl.when(g == 3)
                def _():
                    half(xn + flip, 3, 1, yn, 15).start()

        unit(xn + flip * p, g, yn + flip * p, g)
        return 0

    lax.fori_loop(0, 2 * NG, near, 0)

    d1 = dg - core + 1
    d0 = dg - core

    def hand_on(slot, h, sem):
        half(slot, 2, h, pt, sem).start()
        half(slot, 3, h, pt, sem).start()

    def first_half(slot):
        for t in range(4):
            for k in range(4):
                part[slot % 2, k, :, 256 * t:256 * t + 256] = outer(k, 0, t, (slot, 2, slot, 3))

    def second_half(slot):
        chunks = (slot, 2, slot, 3)
        finish(chunks, lambda k, t: part[slot % 2, k, :, 256 * t:256 * t + 256] + outer(k, 1, t, chunks))

    def far_from():
        arrived(10)
        whole(dg, 0, pt, 11).start()
        whole(dg, 1, pt, 11).start()

    @pl.when(core == 1)
    def _():
        def far(q, _):
            @pl.when(q == 0)
            def _():
                far_from()

            @pl.when(q == 1)
            def _():
                arrived_halves(12)
                hand_on(d1, 0, 12)
                first_half(d1)
                arrived(11)

            @pl.when(q == 2)
            def _():
                arrived_halves(13)
                hand_on(d1, 1, 13)
                second_half(d1)
                arrived_halves(15)
                hand_on(d0, 1, 15)
                arrived_halves(14)

            slot = d1 - (q + 1) // 2
            g = 2 * (q // 2)
            unit(slot, g, slot, g + 1)
            return 0

        lax.fori_loop(0, 3, far, 0)

    @pl.when(core == 0)
    def _():
        def far(q, _):
            @pl.when(q == 0)
            def _():
                far_from()

            @pl.when(q == 1)
            def _():
                arrived(11)

            unit(d0 + q, 0, d0 + q, 1)
            return 0

        lax.fori_loop(0, 2, far, 0)

        def first(q, _):
            arrived_halves(12 + 2 * q)

            @pl.when(q == 1)
            def _():
                hand_on(d0, 0, 14)

            first_half(d1 - q)
            return 0

        lax.fori_loop(0, 2, first, 0)

        def second(q, _):
            arrived_halves(13 + 2 * q)
            second_half(d1 - q)
            return 0

        lax.fori_loop(0, 2, second, 0)

    span(b_buf.at[pl.ds(0, 6)], 0, 0).wait_send()

    @pl.when(core == 1)
    def _():
        span(b_buf.at[pl.ds(0, 2), pl.ds(0, 3)], 1, 0).wait_send()

    @pl.when(core == 0)
    def _():
        span(b_buf.at[0, pl.ds(0, 2)], 1, 0).wait_send()


def local_update(z, m, lns, lno, wa, ba, wb, bb, wo, bo):
    hbm = pl.BlockSpec(memory_space=pltpu.HBM)
    vmem = pl.BlockSpec(memory_space=pltpu.VMEM)
    args = (z.reshape(NL, N // J, J, Z), m.transpose(1, 2, 0), lns.reshape(1, M), lno.reshape(1, M),
            wa.T, ba.reshape(1, H), wb.T, bb.reshape(1, H), wo, bo.reshape(1, Z))
    out = pl.pallas_call(
        kernel,
        out_shape=jax.ShapeDtypeStruct((NL, N // J, J, Z), BF16),
        in_specs=[hbm] * len(args),
        out_specs=vmem,
        scratch_shapes=[
            pltpu.VMEM((8, NG, 2, HQ, CR, 128), BF16),
            pltpu.VMEM((2, HQ, NL * H, 128), BF16),
            pltpu.VMEM((4, NL * H // 128, S, 128), BF16),
            pltpu.VMEM((NL, M, S), BF16),
            pltpu.VMEM((HS // 128, CR, 128), F32),
            pltpu.VMEM((4, 8, 2 * KR, 128), BF16),
            pltpu.VMEM((H * H, Z), BF16),
            pltpu.VMEM((H * H, Z), F32),
            pltpu.VMEM((4, H * H, Z), BF16),
            pltpu.VMEM((NL, N // J, J, Z), BF16),
            pltpu.VMEM((3, M, 128), F32),
            pltpu.VMEM((1, M), BF16),
            pltpu.VMEM((1, M), BF16),
            pltpu.VMEM((H, M), BF16),
            pltpu.VMEM((1, H), BF16),
            pltpu.VMEM((H, M), BF16),
            pltpu.VMEM((1, H), BF16),
            pltpu.VMEM((1, Z), BF16),
            pltpu.VMEM((2, 4, 2 * KR, NL * H), F32),
            pltpu.SemaphoreType.DMA((14,)),
            pltpu.SemaphoreType.DMA((2,)),
            pltpu.SemaphoreType.DMA((16,)),
        ],
        compiler_params=pltpu.CompilerParams(
            collective_id=0, has_side_effects=True, vmem_limit_bytes=48 * 1024 * 1024),
    )(*(pltpu.with_memory_space_constraint(x, pltpu.HBM) for x in args))
    return out.reshape(NL, N, Z)


def solution(mesh):
    row, col, rep = P(("batch", "dap")), P(None, ("batch", "dap")), P()
    return jax.shard_map(local_update, mesh=mesh, in_specs=(row, col) + (rep,) * 8, out_specs=row, check_vma=False)
```

```python
import jax
import jax.numpy as jnp
from jax import lax
from jax.experimental import pallas as pl
from jax.experimental.pallas import tpu as pltpu
from jax.sharding import PartitionSpec as P

MESH = pl.DeviceIdType.MESH
F32, BF16 = jnp.float32, jnp.bfloat16
LN_EPS = 1e-5
S, NL, M, H, N, Z = 512, 32, 64, 32, 256, 128
J = 8
NG = NL // J
CR = H * J
KR = CR // 4
HS = S // 2
HQ = HS // 128
NT = (((1,), (1,)), ((), ()))
NN = (((1,), (0,)), ((), ()))


def dot(x, y, dims=NN):
    return lax.dot_general(x, y, dims, preferred_element_type=F32)


def onehot(rows, cols, fn):
    r = lax.broadcasted_iota(jnp.int32, (rows, cols), 0)
    c = lax.broadcasted_iota(jnp.int32, (rows, cols), 1)
    return jnp.where(fn(r) == c, 1.0, 0.0).astype(BF16)


def project(lhs2, w_v, v):
    return dot(jnp.concatenate([lhs2[v, e] for e in range(8)], axis=1), w_v[v])


def kernel(z_hbm, m_hbm, lns_hbm, lno_hbm, wa_hbm, ba_hbm, wb_hbm, bb_hbm, wo_hbm, bo_hbm,
           out_ref, lhs2, w_v, z_buf, bias_ref,
           b_buf, a_t, a_v, m_buf, b_f32, w_buf, w_f32, par,
           lns_ref, lno_ref, wa_ref, ba_ref, wb_ref, bb_ref, bo_ref,
           part, recv_sem, in_sem, send_sem):
    me = lax.axis_index("dap")
    core = me % 2
    xbit = (me // 2) % 2
    pt = me + 1 - 2 * core
    flip = pt - me
    xn = me + 2 - 4 * xbit
    yn = (me + 4) % 8
    dg = (xn + 4) % 8

    barrier = pltpu.get_barrier_semaphore()
    for dev in (pt, xn, yn):
        pl.semaphore_signal(barrier, inc=1, device_id={"dap": dev}, device_id_type=MESH)

    def m_part(i):
        part_of = pl.ds(0, J), slice(None), pl.ds(i * 128, 128)
        return pltpu.make_async_copy(m_hbm.at[part_of], m_buf.at[part_of], in_sem.at[i])

    m_rest = pltpu.make_async_copy(m_hbm.at[pl.ds(J, NL - J)], m_buf.at[pl.ds(J, NL - J)], in_sem.at[12])
    w_copy = pltpu.make_async_copy(wo_hbm, w_buf, in_sem.at[13])
    z_copy = pltpu.make_async_copy(z_hbm, z_buf, in_sem.at[4])
    small = [pltpu.make_async_copy(src, dst, in_sem.at[5 + i]) for i, (src, dst) in enumerate((
        (lns_hbm, lns_ref), (lno_hbm, lno_ref), (wa_hbm, wa_ref), (ba_hbm, ba_ref),
        (wb_hbm, wb_ref), (bb_hbm, bb_ref), (bo_hbm, bo_ref)))]
    m_part(0).start()
    for copy in small:
        copy.start()
    for i in range(1, S // 128):
        m_part(i).start()
    m_rest.start()
    w_copy.start()
    z_copy.start()

    def whole(slot, g, dev, sem):
        return pltpu.make_async_remote_copy(
            src_ref=b_buf.at[slot, g], dst_ref=b_buf.at[slot, g], send_sem=send_sem.at[0],
            recv_sem=recv_sem.at[sem], device_id={"dap": dev}, device_id_type=MESH)

    def half(slot, g, h, dev, sem, k=1):
        return pltpu.make_async_remote_copy(
            src_ref=b_buf.at[slot, g, h], dst_ref=b_buf.at[slot, g, h], send_sem=send_sem.at[k],
            recv_sem=recv_sem.at[sem], device_id={"dap": dev}, device_id_type=MESH)

    def span(ref, k, sem):
        return pltpu.make_async_remote_copy(
            src_ref=ref, dst_ref=ref, send_sem=send_sem.at[k], recv_sem=recv_sem.at[sem],
            device_id={"dap": pt}, device_id_type=MESH)

    def arrived(sem):
        span(b_buf.at[0, pl.ds(0, 2)], 0, sem).wait_recv()

    def arrived_halves(sem):
        span(b_buf.at[0, 0], 0, sem).wait_recv()

    for copy in small:
        copy.wait()

    def column(row, width):
        return jnp.broadcast_to(row.astype(F32).reshape(1, width), (128, width)).astype(BF16)

    eye = onehot(M, M, lambda r: r)
    order = onehot(2 * H, 2 * H, lambda r: jnp.where(r < H, r, H + 4 * ((r - H) % 8) + (r - H) // 8))
    w_ab = dot(order, jnp.concatenate([wa_ref[...], wb_ref[...]], axis=0)).astype(BF16)
    par[0] = dot(eye, column(lns_ref[...], M), NT)
    par[1] = dot(eye, column(lno_ref[...], M), NT)
    bias = jnp.concatenate([column(ba_ref[...], H), column(bb_ref[...], H)], axis=1)
    par[2] = dot(order, bias, NT)

    def make(g, h, q0, nq):
        def lanes(i):
            return jnp.concatenate([par[i]] * nq, axis=1)

        lo = HS * h + 128 * q0
        for n in range(J):
            x = m_buf[g * J + n, :, lo:lo + 128 * nq].astype(F32)
            mean = jnp.sum(x, axis=0, keepdims=True) * (1.0 / M)
            x = x - mean
            var = jnp.sum(x * x, axis=0, keepdims=True) * (1.0 / M)
            x = x * lax.rsqrt(var + LN_EPS)
            x = (x * lanes(0) + lanes(1)).astype(BF16)
            r = dot(w_ab, x) + lanes(2)
            for q in range(nq):
                rq = r[:, 128 * q:128 * q + 128]
                a_t[h, q0 + q, pl.ds((g * J + n) * H, H), :] = rq[:H].astype(BF16)
                b_f32[q0 + q, pl.ds(n, H, stride=J), :] = rq[H:]
        for q in range(q0, q0 + nq):
            b_buf[me, g, h, q] = b_f32[q].astype(BF16)

    for i in range(S // 128):
        m_part(i).wait()
        h, q = i // HQ, i % HQ
        make(0, h, q, 1)
        if i == 0:
            pl.semaphore_wait(barrier, 3)
        for dev, sem in ((xn, 2), (yn, 2), (pt, 0)):
            piece = b_buf.at[me, 0, h, q]
            pltpu.make_async_remote_copy(
                src_ref=piece, dst_ref=piece, send_sem=send_sem.at[0], recv_sem=recv_sem.at[sem],
                device_id={"dap": dev}, device_id_type=MESH).start()
    m_rest.wait()

    def produce(g, _):
        for h in range(2):
            make(g, h, 0, HQ)
        whole(me, g, xn, 2 + g).start()
        whole(me, g, yn, 2 + g).start()
        whole(me, g, pt, g // 2).start()
        return 0

    lax.fori_loop(1, NG, produce, 0)

    eye256 = onehot(256, 256, lambda r: r)
    for t in range(4):
        for k in range(4):
            for h in range(2):
                rows = jnp.concatenate([jnp.concatenate(
                    [a_t[h, q, pl.ds((8 * t + 4 * gg + (m + k) % 4) * H, H), :] for gg in range(2) for m in range(4)],
                    axis=0) for q in range(HQ)], axis=1)
                block = dot(eye256, rows, NT).astype(BF16)
                for gg in range(2):
                    a_v[k, 2 * t + gg, HS * h:HS * h + HS, :] = block[:, 128 * gg:128 * gg + 128]

    w_copy.wait()
    w_f32[...] = w_buf[...].astype(F32)
    for d in range(H):
        block = w_f32[pl.ds(d, H, stride=H), :].astype(BF16)
        for v in range(4):
            w_v[v, pl.ds((d // 4) * 128 + ((v - d) % 4) * H, H), :] = block
    z_copy.wait()

    bias_out = bo_ref[...].astype(F32).reshape(1, Z)
    bias_ref[...] = jnp.broadcast_to(bias_out, (8, Z))
    lane = lax.broadcasted_iota(jnp.int32, (2 * KR, 128), 1) // H
    even = lane % 2 == 0
    ends = (lane == 0) | (lane == 3)
    low = lane < 2

    def pair(slot_a, g_a, slot_b, g_b, k, h):
        return jnp.concatenate([jnp.concatenate(
            [b_buf[slot_a, g_a, h, q, KR * k:KR * k + KR, :], b_buf[slot_b, g_b, h, q, KR * k:KR * k + KR, :]],
            axis=0) for q in range(HQ)], axis=1)

    def a_cols(k, t, lo, n):
        return jnp.concatenate([a_v[k, 2 * t + gg, lo:lo + n, :] for gg in range(2)], axis=1)

    def outer(k, h, t, chunks):
        return dot(pair(*chunks, k, h), a_cols(k, t, HS * h, HS))

    def regroup(product):
        for t in range(4):
            o = [product(k, t) * (1.0 / S) for k in range(4)]
            q = [[None, None] for _ in range(4)]
            for gg in range(2):
                p = [x[:, 128 * gg:128 * gg + 128] for x in o]
                e0, f0 = jnp.where(even, p[0], p[1]), jnp.where(even, p[2], p[3])
                e1, f1 = jnp.where(even, p[1], p[0]), jnp.where(even, p[3], p[2])
                q[0][gg] = jnp.where(ends, e0, f0)
                q[2][gg] = jnp.where(ends, f0, e0)
                q[1][gg] = jnp.where(low, e1, f1)
                q[3][gg] = jnp.where(low, f1, e1)
            for v in range(4):
                for c in range(2):
                    for e in range(8):
                        r0 = c * KR + e * J
                        lhs2[v, e, c * KR + 16 * t:c * KR + 16 * t + 16, :] = jnp.concatenate(
                            [q[v][0][r0:r0 + J], q[v][1][r0:r0 + J]], axis=0).astype(BF16)

    def write(slot_a, g_a, slot_b, g_b):
        jc = (slot_a * NG + g_a, slot_b * NG + g_b)
        for v in range(4):
            u = project(lhs2, w_v, v) + bias_out
            for c in range(2):
                for G in range(8):
                    i = 4 * G + v
                    r0 = c * KR + G * J
                    out_ref[i, jc[c]] = (z_buf[i, jc[c]].astype(F32) + u[r0:r0 + J]).astype(BF16)

    def regroup_whole(*chunks):
        lhs = [jnp.concatenate([pair(*chunks, k, h) for h in range(2)], axis=1) for k in range(4)]
        regroup(lambda k, t: dot(lhs[k], a_cols(k, t, 0, S)))

    def regroup_second(slot):
        regroup(lambda k, t: part[slot % 2, k, :, 256 * t:256 * t + 256] + outer(k, 1, t, (slot, 2, slot, 3)))

    def unit(*chunks):
        regroup_whole(*chunks)
        write(*chunks)

    def local(s, _):
        slot = me + flip * (s // 2)
        g = 2 * (s % 2)

        @pl.when(s >= 2)
        def _():
            arrived(s % 2)

        unit(slot, g, slot, g + 1)
        return 0

    lax.fori_loop(0, 4, local, 0)

    def near(s, _):
        g = s // 2
        p = s % 2

        @pl.when(p == 0)
        def _():
            arrived(2 + g)
            for gc in range(NG):
                @pl.when(g == gc)
                def _():
                    slot, dev = (yn, xn) if gc % 2 == 0 else (xn, yn)
                    if gc < 2:
                        whole(slot, gc, dev, 10).start()
                    else:
                        @pl.when(core == 1)
                        def _():
                            half(slot, gc, 0, dev, 12).start()
                            half(slot, gc, 1, dev, 13).start()

                        @pl.when(core == 0)
                        def _():
                            half(slot, gc, 0, dev, 14).start()

            whole(xn, g, pt, 6 + g).start()
            whole(yn, g, pt, 6 + g).start()

        @pl.when(p == 1)
        def _():
            arrived(6 + g)

            @pl.when(core == 1)
            def _():
                @pl.when(g == 2)
                def _():
                    half(yn + flip, 2, 1, xn, 15).start()

                @pl.when(g == 3)
                def _():
                    half(xn + flip, 3, 1, yn, 15).start()

        unit(xn + flip * p, g, yn + flip * p, g)
        return 0

    lax.fori_loop(0, 2 * NG, near, 0)

    d1 = dg - core + 1
    d0 = dg - core

    def hand_on(slot, h, sem):
        half(slot, 2, h, pt, sem).start()
        half(slot, 3, h, pt, sem).start()

    def first_half(slot):
        for t in range(4):
            for k in range(4):
                part[slot % 2, k, :, 256 * t:256 * t + 256] = outer(k, 0, t, (slot, 2, slot, 3))

    def second_half(slot):
        regroup_second(slot)
        write(slot, 2, slot, 3)

    def far_from():
        arrived(10)
        whole(dg, 0, pt, 11).start()
        whole(dg, 1, pt, 11).start()

    @pl.when(core == 1)
    def _():
        def far(q, _):
            @pl.when(q == 0)
            def _():
                far_from()

            @pl.when(q == 1)
            def _():
                arrived_halves(12)
                hand_on(d1, 0, 12)
                first_half(d1)
                arrived(11)

            unit(d1 - q, 0, d1 - q, 1)
            return 0

        lax.fori_loop(0, 2, far, 0)
        arrived_halves(13)
        hand_on(d1, 1, 13)
        second_half(d1)
        arrived_halves(15)
        hand_on(d0, 1, 15)
        arrived_halves(14)
        regroup_whole(d0, 2, d0, 3)

    @pl.when(core == 0)
    def _():
        def far(q, _):
            @pl.when(q == 0)
            def _():
                far_from()

            @pl.when(q == 1)
            def _():
                arrived(11)

            unit(d0 + q, 0, d0 + q, 1)
            return 0

        lax.fori_loop(0, 2, far, 0)

        def first(q, _):
            arrived_halves(12 + 2 * q)

            @pl.when(q == 1)
            def _():
                hand_on(d0, 0, 14)

            first_half(d1 - q)
            return 0

        lax.fori_loop(0, 2, first, 0)

        arrived_halves(13)
        second_half(d1)
        arrived_halves(15)
        regroup_second(d0)

    span(b_buf.at[pl.ds(0, 6)], 0, 0).wait_send()

    @pl.when(core == 1)
    def _():
        span(b_buf.at[pl.ds(0, 2), pl.ds(0, 3)], 1, 0).wait_send()

    @pl.when(core == 0)
    def _():
        span(b_buf.at[0, pl.ds(0, 2)], 1, 0).wait_send()


def last_kernel(out_ref, lhs2, w_v, z_buf, bias_ref, out_hbm, tail, sem):
    me = lax.axis_index("dap")
    slot = 6 - me // 2 * 2
    for chip in range(4):
        @pl.when(me // 2 == chip)
        def _():
            hole = NG * (6 - 2 * chip) + 2
            for lo, n in ((0, hole), (hole + 2, N // J - hole - 2)):
                pltpu.make_async_copy(
                    out_ref.at[:, pl.ds(lo, n)], out_hbm.at[:, pl.ds(lo, n)], sem.at[0]).start()

    first = NG * slot + 2
    for v in range(4):
        u = project(lhs2, w_v, v) + bias_ref[:1, :]
        for c in range(2):
            for G in range(8):
                i = 4 * G + v
                r0 = c * KR + G * J
                tail[i, c] = (z_buf[i, first + c].astype(F32) + u[r0:r0 + J]).astype(BF16)
    rest = pltpu.make_async_copy(tail, out_hbm.at[:, pl.ds(first, 2)], sem.at[1])
    rest.start()
    done = out_ref.at[:, pl.ds(0, N // J - 2)]
    pltpu.make_async_copy(done, out_hbm.at[:, pl.ds(0, N // J - 2)], sem.at[0]).wait()
    rest.wait()


def local_update(z, m, lns, lno, wa, ba, wb, bb, wo, bo):
    hbm = pl.BlockSpec(memory_space=pltpu.HBM)
    vmem = pl.BlockSpec(memory_space=pltpu.VMEM)
    args = (z.reshape(NL, N // J, J, Z), m.transpose(1, 2, 0), lns.reshape(1, M), lno.reshape(1, M),
            wa.T, ba.reshape(1, H), wb.T, bb.reshape(1, H), wo, bo.reshape(1, Z))
    rows = jax.ShapeDtypeStruct((NL, N // J, J, Z), BF16)
    def scoped(*refs):
        pl.run_scoped(lambda in_sem, send_sem: kernel(*refs, in_sem, send_sem),
                      pltpu.SemaphoreType.DMA((14,)), pltpu.SemaphoreType.DMA((2,)))

    parts = pl.pallas_call(
        scoped,
        out_shape=(rows, jax.ShapeDtypeStruct((4, 8, 2 * KR, 128), BF16), jax.ShapeDtypeStruct((4, H * H, Z), BF16),
                   rows, jax.ShapeDtypeStruct((8, Z), F32)),
        in_specs=[hbm] * len(args),
        out_specs=(vmem,) * 5,
        scratch_shapes=[
            pltpu.VMEM((8, NG, 2, HQ, CR, 128), BF16),
            pltpu.VMEM((2, HQ, NL * H, 128), BF16),
            pltpu.VMEM((4, NL * H // 128, S, 128), BF16),
            pltpu.VMEM((NL, M, S), BF16),
            pltpu.VMEM((HQ, CR, 128), F32),
            pltpu.VMEM((H * H, Z), BF16),
            pltpu.VMEM((H * H, Z), F32),
            pltpu.VMEM((3, M, 128), F32),
            pltpu.VMEM((1, M), BF16),
            pltpu.VMEM((1, M), BF16),
            pltpu.VMEM((H, M), BF16),
            pltpu.VMEM((1, H), BF16),
            pltpu.VMEM((H, M), BF16),
            pltpu.VMEM((1, H), BF16),
            pltpu.VMEM((1, Z), BF16),
            pltpu.VMEM((2, 4, 2 * KR, NL * H), F32),
            pltpu.SemaphoreType.DMA((16,)),
        ],
        compiler_params=pltpu.CompilerParams(
            collective_id=0, has_side_effects=True, vmem_limit_bytes=36 * 1024 * 1024),
    )(*(pltpu.with_memory_space_constraint(x, pltpu.HBM) for x in args))
    out = pl.pallas_call(
        last_kernel,
        out_shape=rows,
        in_specs=[vmem] * 5,
        out_specs=hbm,
        scratch_shapes=[pltpu.VMEM((NL, 2, J, Z), BF16), pltpu.SemaphoreType.DMA((2,))],
        compiler_params=pltpu.CompilerParams(vmem_limit_bytes=4 * 1024 * 1024),
    )(*parts)
    return out.reshape(NL, N, Z)


def solution(mesh):
    row, col, rep = P(("batch", "dap")), P(None, ("batch", "dap")), P()
    return jax.shard_map(local_update, mesh=mesh, in_specs=(row, col) + (rep,) * 8, out_specs=row, check_vma=False)
```

```python
import jax
import jax.numpy as jnp
from jax import lax
from jax.experimental import pallas as pl
from jax.experimental.pallas import tpu as pltpu
from jax.sharding import PartitionSpec as P

MESH = pl.DeviceIdType.MESH
F32, BF16 = jnp.float32, jnp.bfloat16
LN_EPS = 1e-5
S, NL, M, H, N, Z = 512, 32, 64, 32, 256, 128
J = 8
NG = NL // J
CR = H * J
KR = CR // 4
HS = S // 2
HQ = HS // 128
NT = (((1,), (1,)), ((), ()))
NN = (((1,), (0,)), ((), ()))


def dot(x, y, dims=NN):
    return lax.dot_general(x, y, dims, preferred_element_type=F32)


def onehot(rows, cols, fn):
    r = lax.broadcasted_iota(jnp.int32, (rows, cols), 0)
    c = lax.broadcasted_iota(jnp.int32, (rows, cols), 1)
    return jnp.where(fn(r) == c, 1.0, 0.0).astype(BF16)


def project(lhs2, w_v, v):
    return dot(jnp.concatenate([lhs2[v, e] for e in range(8)], axis=1), w_v[v])


def kernel(z_hbm, m_hbm, lns_hbm, lno_hbm, wa_hbm, ba_hbm, wb_hbm, bb_hbm, wo_hbm, bo_hbm,
           out_ref, lhs2, w_v, z_buf, bias_ref,
           b_buf, a_t, a_v, m_buf, b_f32, w_buf, w_f32, par,
           lns_ref, lno_ref, wa_ref, ba_ref, wb_ref, bb_ref, bo_ref,
           part, recv_sem, in_sem, send_sem):
    me = lax.axis_index("dap")
    core = me % 2
    xbit = (me // 2) % 2
    pt = me + 1 - 2 * core
    flip = pt - me
    xn = me + 2 - 4 * xbit
    yn = (me + 4) % 8
    dg = (xn + 4) % 8

    barrier = pltpu.get_barrier_semaphore()
    for dev in (pt, xn, yn):
        pl.semaphore_signal(barrier, inc=1, device_id={"dap": dev}, device_id_type=MESH)

    def m_part(i):
        part_of = pl.ds(0, J), slice(None), pl.ds(i * 128, 128)
        return pltpu.make_async_copy(m_hbm.at[part_of], m_buf.at[part_of], in_sem.at[i])

    m_rest = pltpu.make_async_copy(m_hbm.at[pl.ds(J, NL - J)], m_buf.at[pl.ds(J, NL - J)], in_sem.at[12])
    w_copy = pltpu.make_async_copy(wo_hbm, w_buf, in_sem.at[13])
    z_copy = pltpu.make_async_copy(z_hbm, z_buf, in_sem.at[4])
    small = [pltpu.make_async_copy(src, dst, in_sem.at[5 + i]) for i, (src, dst) in enumerate((
        (lns_hbm, lns_ref), (lno_hbm, lno_ref), (wa_hbm, wa_ref), (ba_hbm, ba_ref),
        (wb_hbm, wb_ref), (bb_hbm, bb_ref), (bo_hbm, bo_ref)))]
    for copy in small:
        copy.start()
    for n in range(0, J, 2):
        part_of = pl.ds(n, 2), slice(None), pl.ds(0, 128)
        pltpu.make_async_copy(m_hbm.at[part_of], m_buf.at[part_of], in_sem.at[0]).start()
    for i in range(1, S // 128):
        m_part(i).start()

    def whole(slot, g, dev, sem):
        return pltpu.make_async_remote_copy(
            src_ref=b_buf.at[slot, g], dst_ref=b_buf.at[slot, g], send_sem=send_sem.at[0],
            recv_sem=recv_sem.at[sem], device_id={"dap": dev}, device_id_type=MESH)

    def half(slot, g, h, dev, sem, k=1):
        return pltpu.make_async_remote_copy(
            src_ref=b_buf.at[slot, g, h], dst_ref=b_buf.at[slot, g, h], send_sem=send_sem.at[k],
            recv_sem=recv_sem.at[sem], device_id={"dap": dev}, device_id_type=MESH)

    def span(ref, k, sem):
        return pltpu.make_async_remote_copy(
            src_ref=ref, dst_ref=ref, send_sem=send_sem.at[k], recv_sem=recv_sem.at[sem],
            device_id={"dap": pt}, device_id_type=MESH)

    def arrived(sem):
        span(b_buf.at[0, pl.ds(0, 2)], 0, sem).wait_recv()

    def arrived_halves(sem):
        span(b_buf.at[0, 0], 0, sem).wait_recv()

    for copy in small:
        copy.wait()

    def column(row, width):
        return jnp.broadcast_to(row.astype(F32).reshape(1, width), (128, width)).astype(BF16)

    eye = onehot(M, M, lambda r: r)
    order = onehot(2 * H, 2 * H, lambda r: jnp.where(r < H, r, H + 4 * ((r - H) % 8) + (r - H) // 8))
    w_ab = dot(order, jnp.concatenate([wa_ref[...], wb_ref[...]], axis=0)).astype(BF16)
    par[0] = dot(eye, column(lns_ref[...], M), NT)
    par[1] = dot(eye, column(lno_ref[...], M), NT)
    bias = jnp.concatenate([column(ba_ref[...], H), column(bb_ref[...], H)], axis=1)
    par[2] = dot(order, bias, NT)

    def make(g, h, q0, nq):
        def lanes(i):
            return jnp.concatenate([par[i]] * nq, axis=1)

        lo = HS * h + 128 * q0
        for n in range(J):
            x = m_buf[g * J + n, :, lo:lo + 128 * nq].astype(F32)
            mean = jnp.sum(x, axis=0, keepdims=True) * (1.0 / M)
            x = x - mean
            var = jnp.sum(x * x, axis=0, keepdims=True) * (1.0 / M)
            x = x * lax.rsqrt(var + LN_EPS)
            x = (x * lanes(0) + lanes(1)).astype(BF16)
            r = dot(w_ab, x) + lanes(2)
            for q in range(nq):
                rq = r[:, 128 * q:128 * q + 128]
                a_t[h, q0 + q, pl.ds((g * J + n) * H, H), :] = rq[:H].astype(BF16)
                b_f32[q0 + q, pl.ds(n, H, stride=J), :] = rq[H:]
        for q in range(q0, q0 + nq):
            b_buf[me, g, h, q] = b_f32[q].astype(BF16)

    for i in range(S // 128):
        m_part(i).wait()
        if i == 0:
            m_rest.start()
            w_copy.start()
            z_copy.start()
        h, q = i // HQ, i % HQ
        make(0, h, q, 1)
        if i == 0:
            pl.semaphore_wait(barrier, 3)
        for dev, sem in ((xn, 2), (yn, 2), (pt, 0)):
            piece = b_buf.at[me, 0, h, q]
            pltpu.make_async_remote_copy(
                src_ref=piece, dst_ref=piece, send_sem=send_sem.at[0], recv_sem=recv_sem.at[sem],
                device_id={"dap": dev}, device_id_type=MESH).start()
    m_rest.wait()

    def produce(g, _):
        for h in range(2):
            make(g, h, 0, HQ)
        whole(me, g, xn, 2 + g).start()
        whole(me, g, yn, 2 + g).start()
        whole(me, g, pt, g // 2).start()
        return 0

    lax.fori_loop(1, NG, produce, 0)

    eye256 = onehot(256, 256, lambda r: r)
    for t in range(4):
        for k in range(4):
            for h in range(2):
                rows = jnp.concatenate([jnp.concatenate(
                    [a_t[h, q, pl.ds((8 * t + 4 * gg + (m + k) % 4) * H, H), :] for gg in range(2) for m in range(4)],
                    axis=0) for q in range(HQ)], axis=1)
                block = dot(eye256, rows, NT).astype(BF16)
                for gg in range(2):
                    a_v[k, 2 * t + gg, HS * h:HS * h + HS, :] = block[:, 128 * gg:128 * gg + 128]

    w_copy.wait()
    w_f32[...] = w_buf[...].astype(F32)
    for d in range(H):
        block = w_f32[pl.ds(d, H, stride=H), :].astype(BF16)
        for v in range(4):
            w_v[v, pl.ds((d // 4) * 128 + ((v - d) % 4) * H, H), :] = block
    z_copy.wait()

    bias_out = bo_ref[...].astype(F32).reshape(1, Z)
    bias_ref[...] = jnp.broadcast_to(bias_out, (8, Z))
    lane = lax.broadcasted_iota(jnp.int32, (2 * KR, 128), 1) // H
    even = lane % 2 == 0
    ends = (lane == 0) | (lane == 3)
    low = lane < 2

    def pair(slot_a, g_a, slot_b, g_b, k, h):
        return jnp.concatenate([jnp.concatenate(
            [b_buf[slot_a, g_a, h, q, KR * k:KR * k + KR, :], b_buf[slot_b, g_b, h, q, KR * k:KR * k + KR, :]],
            axis=0) for q in range(HQ)], axis=1)

    def a_cols(k, t, lo, n):
        return jnp.concatenate([a_v[k, 2 * t + gg, lo:lo + n, :] for gg in range(2)], axis=1)

    def outer(k, h, t, chunks):
        return dot(pair(*chunks, k, h), a_cols(k, t, HS * h, HS))

    def regroup(product):
        for t in range(4):
            o = [product(k, t) * (1.0 / S) for k in range(4)]
            q = [[None, None] for _ in range(4)]
            for gg in range(2):
                p = [x[:, 128 * gg:128 * gg + 128] for x in o]
                e0, f0 = jnp.where(even, p[0], p[1]), jnp.where(even, p[2], p[3])
                e1, f1 = jnp.where(even, p[1], p[0]), jnp.where(even, p[3], p[2])
                q[0][gg] = jnp.where(ends, e0, f0)
                q[2][gg] = jnp.where(ends, f0, e0)
                q[1][gg] = jnp.where(low, e1, f1)
                q[3][gg] = jnp.where(low, f1, e1)
            for v in range(4):
                for c in range(2):
                    for e in range(8):
                        r0 = c * KR + e * J
                        lhs2[v, e, c * KR + 16 * t:c * KR + 16 * t + 16, :] = jnp.concatenate(
                            [q[v][0][r0:r0 + J], q[v][1][r0:r0 + J]], axis=0).astype(BF16)

    def write(slot_a, g_a, slot_b, g_b):
        jc = (slot_a * NG + g_a, slot_b * NG + g_b)
        for v in range(4):
            u = project(lhs2, w_v, v) + bias_out
            for c in range(2):
                for G in range(8):
                    i = 4 * G + v
                    r0 = c * KR + G * J
                    out_ref[i, jc[c]] = (z_buf[i, jc[c]].astype(F32) + u[r0:r0 + J]).astype(BF16)

    def regroup_whole(*chunks):
        lhs = [jnp.concatenate([pair(*chunks, k, h) for h in range(2)], axis=1) for k in range(4)]
        regroup(lambda k, t: dot(lhs[k], a_cols(k, t, 0, S)))

    def regroup_second(slot):
        regroup(lambda k, t: part[slot % 2, k, :, 256 * t:256 * t + 256] + outer(k, 1, t, (slot, 2, slot, 3)))

    def unit(*chunks):
        regroup_whole(*chunks)
        write(*chunks)

    def local(s, _):
        slot = me + flip * (s // 2)
        g = 2 * (s % 2)

        @pl.when(s >= 2)
        def _():
            arrived(s % 2)

        unit(slot, g, slot, g + 1)
        return 0

    lax.fori_loop(0, 4, local, 0)

    def near(s, _):
        g = s // 2
        p = s % 2

        @pl.when(p == 0)
        def _():
            arrived(2 + g)
            for gc in range(NG):
                @pl.when(g == gc)
                def _():
                    slot, dev = (yn, xn) if gc % 2 == 0 else (xn, yn)
                    if gc < 2:
                        whole(slot, gc, dev, 10).start()
                    else:
                        @pl.when(core == 1)
                        def _():
                            half(slot, gc, 0, dev, 12).start()
                            half(slot, gc, 1, dev, 13).start()

                        @pl.when(core == 0)
                        def _():
                            half(slot, gc, 0, dev, 14).start()

            whole(xn, g, pt, 6 + g).start()
            whole(yn, g, pt, 6 + g).start()

        @pl.when(p == 1)
        def _():
            arrived(6 + g)

            @pl.when(core == 1)
            def _():
                @pl.when(g == 2)
                def _():
                    half(yn + flip, 2, 1, xn, 15).start()

                @pl.when(g == 3)
                def _():
                    half(xn + flip, 3, 1, yn, 15).start()

        unit(xn + flip * p, g, yn + flip * p, g)
        return 0

    lax.fori_loop(0, 2 * NG, near, 0)

    d1 = dg - core + 1
    d0 = dg - core

    def hand_on(slot, h, sem):
        half(slot, 2, h, pt, sem).start()
        half(slot, 3, h, pt, sem).start()

    def first_half(slot):
        for t in range(4):
            for k in range(4):
                part[slot % 2, k, :, 256 * t:256 * t + 256] = outer(k, 0, t, (slot, 2, slot, 3))

    def second_half(slot):
        regroup_second(slot)
        write(slot, 2, slot, 3)

    def far_from():
        arrived(10)
        whole(dg, 0, pt, 11).start()
        whole(dg, 1, pt, 11).start()

    @pl.when(core == 1)
    def _():
        def far(q, _):
            @pl.when(q == 0)
            def _():
                far_from()

            @pl.when(q == 1)
            def _():
                arrived_halves(12)
                hand_on(d1, 0, 12)
                first_half(d1)
                arrived(11)

            unit(d1 - q, 0, d1 - q, 1)
            return 0

        lax.fori_loop(0, 2, far, 0)
        arrived_halves(13)
        hand_on(d1, 1, 13)
        second_half(d1)
        arrived_halves(15)
        hand_on(d0, 1, 15)
        arrived_halves(14)
        regroup_whole(d0, 2, d0, 3)

    @pl.when(core == 0)
    def _():
        def far(q, _):
            @pl.when(q == 0)
            def _():
                far_from()

            @pl.when(q == 1)
            def _():
                arrived(11)

            unit(d0 + q, 0, d0 + q, 1)
            return 0

        lax.fori_loop(0, 2, far, 0)

        def first(q, _):
            arrived_halves(12 + 2 * q)

            @pl.when(q == 1)
            def _():
                hand_on(d0, 0, 14)

            first_half(d1 - q)
            return 0

        lax.fori_loop(0, 2, first, 0)

        arrived_halves(13)
        second_half(d1)
        arrived_halves(15)
        regroup_second(d0)

    span(b_buf.at[pl.ds(0, 6)], 0, 0).wait_send()

    @pl.when(core == 1)
    def _():
        span(b_buf.at[pl.ds(0, 2), pl.ds(0, 3)], 1, 0).wait_send()

    @pl.when(core == 0)
    def _():
        span(b_buf.at[0, pl.ds(0, 2)], 1, 0).wait_send()


def last_kernel(out_ref, lhs2, w_v, z_buf, bias_ref, out_hbm, tail, sem):
    me = lax.axis_index("dap")
    slot = 6 - me // 2 * 2
    for chip in range(4):
        @pl.when(me // 2 == chip)
        def _():
            hole = NG * (6 - 2 * chip) + 2
            for lo, n in ((0, hole), (hole + 2, N // J - hole - 2)):
                pltpu.make_async_copy(
                    out_ref.at[:, pl.ds(lo, n)], out_hbm.at[:, pl.ds(lo, n)], sem.at[0]).start()

    first = NG * slot + 2
    for v in range(4):
        u = project(lhs2, w_v, v) + bias_ref[:1, :]
        for c in range(2):
            for G in range(8):
                i = 4 * G + v
                r0 = c * KR + G * J
                tail[i, c] = (z_buf[i, first + c].astype(F32) + u[r0:r0 + J]).astype(BF16)
    rest = pltpu.make_async_copy(tail, out_hbm.at[:, pl.ds(first, 2)], sem.at[1])
    rest.start()
    done = out_ref.at[:, pl.ds(0, N // J - 2)]
    pltpu.make_async_copy(done, out_hbm.at[:, pl.ds(0, N // J - 2)], sem.at[0]).wait()
    rest.wait()


def local_update(z, m, lns, lno, wa, ba, wb, bb, wo, bo):
    hbm = pl.BlockSpec(memory_space=pltpu.HBM)
    vmem = pl.BlockSpec(memory_space=pltpu.VMEM)
    args = (z.reshape(NL, N // J, J, Z), m.transpose(1, 2, 0), lns.reshape(1, M), lno.reshape(1, M),
            wa.T, ba.reshape(1, H), wb.T, bb.reshape(1, H), wo, bo.reshape(1, Z))
    rows = jax.ShapeDtypeStruct((NL, N // J, J, Z), BF16)
    def scoped(*refs):
        pl.run_scoped(lambda in_sem, send_sem: kernel(*refs, in_sem, send_sem),
                      pltpu.SemaphoreType.DMA((14,)), pltpu.SemaphoreType.DMA((2,)))

    parts = pl.pallas_call(
        scoped,
        out_shape=(rows, jax.ShapeDtypeStruct((4, 8, 2 * KR, 128), BF16), jax.ShapeDtypeStruct((4, H * H, Z), BF16),
                   rows, jax.ShapeDtypeStruct((8, Z), F32)),
        in_specs=[hbm] * len(args),
        out_specs=(vmem,) * 5,
        scratch_shapes=[
            pltpu.VMEM((8, NG, 2, HQ, CR, 128), BF16),
            pltpu.VMEM((2, HQ, NL * H, 128), BF16),
            pltpu.VMEM((4, NL * H // 128, S, 128), BF16),
            pltpu.VMEM((NL, M, S), BF16),
            pltpu.VMEM((HQ, CR, 128), F32),
            pltpu.VMEM((H * H, Z), BF16),
            pltpu.VMEM((H * H, Z), F32),
            pltpu.VMEM((3, M, 128), F32),
            pltpu.VMEM((1, M), BF16),
            pltpu.VMEM((1, M), BF16),
            pltpu.VMEM((H, M), BF16),
            pltpu.VMEM((1, H), BF16),
            pltpu.VMEM((H, M), BF16),
            pltpu.VMEM((1, H), BF16),
            pltpu.VMEM((1, Z), BF16),
            pltpu.VMEM((2, 4, 2 * KR, NL * H), F32),
            pltpu.SemaphoreType.DMA((16,)),
        ],
        compiler_params=pltpu.CompilerParams(
            collective_id=0, has_side_effects=True, vmem_limit_bytes=36 * 1024 * 1024),
    )(*(pltpu.with_memory_space_constraint(x, pltpu.HBM) for x in args))
    out = pl.pallas_call(
        last_kernel,
        out_shape=rows,
        in_specs=[vmem] * 5,
        out_specs=hbm,
        scratch_shapes=[pltpu.VMEM((NL, 2, J, Z), BF16), pltpu.SemaphoreType.DMA((2,))],
        compiler_params=pltpu.CompilerParams(vmem_limit_bytes=4 * 1024 * 1024),
    )(*parts)
    return out.reshape(NL, N, Z)


def solution(mesh):
    row, col, rep = P(("batch", "dap")), P(None, ("batch", "dap")), P()
    return jax.shard_map(local_update, mesh=mesh, in_specs=(row, col) + (rep,) * 8, out_specs=row, check_vma=False)
```

```python
import jax
import jax.numpy as jnp
from jax import lax
from jax.experimental import pallas as pl
from jax.experimental.pallas import tpu as pltpu
from jax.sharding import PartitionSpec as P

MESH = pl.DeviceIdType.MESH
F32, BF16 = jnp.float32, jnp.bfloat16
LN_EPS = 1e-5
S, NL, M, H, N, Z = 512, 32, 64, 32, 256, 128
J = 8
NG = NL // J
CR = H * J
KR = CR // 4
HS = S // 2
EARLY = 2
HQ = HS // 128
NT = (((1,), (1,)), ((), ()))
NN = (((1,), (0,)), ((), ()))


def dot(x, y, dims=NN):
    return lax.dot_general(x, y, dims, preferred_element_type=F32)


def onehot(rows, cols, fn):
    r = lax.broadcasted_iota(jnp.int32, (rows, cols), 0)
    c = lax.broadcasted_iota(jnp.int32, (rows, cols), 1)
    return jnp.where(fn(r) == c, 1.0, 0.0).astype(BF16)


def a_cols(a_v, k, t, lo, n):
    return jnp.concatenate([a_v[k, 2 * t + gg, lo:lo + n, :] for gg in range(2)], axis=1)


def regroup(lhs2, steps, product):
    lane = lax.broadcasted_iota(jnp.int32, (2 * KR, 128), 1) // H
    even = lane % 2 == 0
    ends = (lane == 0) | (lane == 3)
    low = lane < 2
    for t in steps:
        o = [product(k, t) * (1.0 / S) for k in range(4)]
        q = [[None, None] for _ in range(4)]
        for gg in range(2):
            p = [x[:, 128 * gg:128 * gg + 128] for x in o]
            e0, f0 = jnp.where(even, p[0], p[1]), jnp.where(even, p[2], p[3])
            e1, f1 = jnp.where(even, p[1], p[0]), jnp.where(even, p[3], p[2])
            q[0][gg] = jnp.where(ends, e0, f0)
            q[2][gg] = jnp.where(ends, f0, e0)
            q[1][gg] = jnp.where(low, e1, f1)
            q[3][gg] = jnp.where(low, f1, e1)
        for v in range(4):
            for c in range(2):
                for e in range(8):
                    r0 = c * KR + e * J
                    lhs2[v, e, c * KR + 16 * t:c * KR + 16 * t + 16, :] = jnp.concatenate(
                        [q[v][0][r0:r0 + J], q[v][1][r0:r0 + J]], axis=0).astype(BF16)


def project(lhs2, w_v, v, later=None):
    def rows(e):
        if later is None:
            return lhs2[v, e]
        return jnp.concatenate([x for c in range(2) for x in (
            lhs2[v, e, c * KR:c * KR + 16 * EARLY, :], later[v, e, c * KR + 16 * EARLY:c * KR + KR, :])], axis=0)

    return dot(jnp.concatenate([rows(e) for e in range(8)], axis=1), w_v[v])


def kernel(z_hbm, m_hbm, lns_hbm, lno_hbm, wa_hbm, ba_hbm, wb_hbm, bb_hbm, wo_hbm, bo_hbm,
           out_ref, lhs2, w_v, z_buf, bias_ref, a_v, part0, b_last,
           b_buf, a_t, m_buf, b_f32, w_buf, w_f32, par,
           lns_ref, lno_ref, wa_ref, ba_ref, wb_ref, bb_ref, bo_ref,
           part1, recv_sem, in_sem, send_sem):
    me = lax.axis_index("dap")
    core = me % 2
    xbit = (me // 2) % 2
    pt = me + 1 - 2 * core
    flip = pt - me
    xn = me + 2 - 4 * xbit
    yn = (me + 4) % 8
    dg = (xn + 4) % 8

    barrier = pltpu.get_barrier_semaphore()
    for dev in (pt, xn, yn):
        pl.semaphore_signal(barrier, inc=1, device_id={"dap": dev}, device_id_type=MESH)

    def m_part(i):
        part_of = pl.ds(0, J), slice(None), pl.ds(i * 128, 128)
        return pltpu.make_async_copy(m_hbm.at[part_of], m_buf.at[part_of], in_sem.at[i])

    m_rest = pltpu.make_async_copy(m_hbm.at[pl.ds(J, NL - J)], m_buf.at[pl.ds(J, NL - J)], in_sem.at[12])
    w_copy = pltpu.make_async_copy(wo_hbm, w_buf, in_sem.at[13])
    z_copy = pltpu.make_async_copy(z_hbm, z_buf, in_sem.at[4])
    small = [pltpu.make_async_copy(src, dst, in_sem.at[5 + i]) for i, (src, dst) in enumerate((
        (lns_hbm, lns_ref), (lno_hbm, lno_ref), (wa_hbm, wa_ref), (ba_hbm, ba_ref),
        (wb_hbm, wb_ref), (bb_hbm, bb_ref), (bo_hbm, bo_ref)))]
    for copy in small:
        copy.start()
    for n in range(0, J, 2):
        part_of = pl.ds(n, 2), slice(None), pl.ds(0, 128)
        pltpu.make_async_copy(m_hbm.at[part_of], m_buf.at[part_of], in_sem.at[0]).start()
    for i in range(1, S // 128):
        m_part(i).start()

    def whole(slot, g, dev, sem):
        return pltpu.make_async_remote_copy(
            src_ref=b_buf.at[slot, g], dst_ref=b_buf.at[slot, g], send_sem=send_sem.at[0],
            recv_sem=recv_sem.at[sem], device_id={"dap": dev}, device_id_type=MESH)

    def half(slot, g, h, dev, sem, k=1):
        return pltpu.make_async_remote_copy(
            src_ref=b_buf.at[slot, g, h], dst_ref=b_buf.at[slot, g, h], send_sem=send_sem.at[k],
            recv_sem=recv_sem.at[sem], device_id={"dap": dev}, device_id_type=MESH)

    def span(ref, k, sem):
        return pltpu.make_async_remote_copy(
            src_ref=ref, dst_ref=ref, send_sem=send_sem.at[k], recv_sem=recv_sem.at[sem],
            device_id={"dap": pt}, device_id_type=MESH)

    def arrived(sem):
        span(b_buf.at[0, pl.ds(0, 2)], 0, sem).wait_recv()

    def arrived_halves(sem):
        span(b_buf.at[0, 0], 0, sem).wait_recv()

    for copy in small:
        copy.wait()

    def column(row, width):
        return jnp.broadcast_to(row.astype(F32).reshape(1, width), (128, width)).astype(BF16)

    eye = onehot(M, M, lambda r: r)
    order = onehot(2 * H, 2 * H, lambda r: jnp.where(r < H, r, H + 4 * ((r - H) % 8) + (r - H) // 8))
    w_ab = dot(order, jnp.concatenate([wa_ref[...], wb_ref[...]], axis=0)).astype(BF16)
    par[0] = dot(eye, column(lns_ref[...], M), NT)
    par[1] = dot(eye, column(lno_ref[...], M), NT)
    bias = jnp.concatenate([column(ba_ref[...], H), column(bb_ref[...], H)], axis=1)
    par[2] = dot(order, bias, NT)

    def make(g, h, q0, nq):
        def lanes(i):
            return jnp.concatenate([par[i]] * nq, axis=1)

        lo = HS * h + 128 * q0
        for n in range(J):
            x = m_buf[g * J + n, :, lo:lo + 128 * nq].astype(F32)
            mean = jnp.sum(x, axis=0, keepdims=True) * (1.0 / M)
            x = x - mean
            var = jnp.sum(x * x, axis=0, keepdims=True) * (1.0 / M)
            x = x * lax.rsqrt(var + LN_EPS)
            x = (x * lanes(0) + lanes(1)).astype(BF16)
            r = dot(w_ab, x) + lanes(2)
            for q in range(nq):
                rq = r[:, 128 * q:128 * q + 128]
                a_t[h, q0 + q, pl.ds((g * J + n) * H, H), :] = rq[:H].astype(BF16)
                b_f32[q0 + q, pl.ds(n, H, stride=J), :] = rq[H:]
        for q in range(q0, q0 + nq):
            b_buf[me, g, h, q] = b_f32[q].astype(BF16)

    for i in range(S // 128):
        m_part(i).wait()
        if i == 0:
            m_rest.start()
            w_copy.start()
            z_copy.start()
        h, q = i // HQ, i % HQ
        make(0, h, q, 1)
        if i == 0:
            pl.semaphore_wait(barrier, 3)
        for dev, sem in ((xn, 2), (yn, 2), (pt, 0)):
            piece = b_buf.at[me, 0, h, q]
            pltpu.make_async_remote_copy(
                src_ref=piece, dst_ref=piece, send_sem=send_sem.at[0], recv_sem=recv_sem.at[sem],
                device_id={"dap": dev}, device_id_type=MESH).start()
    m_rest.wait()

    def produce(g, _):
        for h in range(2):
            make(g, h, 0, HQ)
        whole(me, g, xn, 2 + g).start()
        whole(me, g, yn, 2 + g).start()
        whole(me, g, pt, g // 2).start()
        return 0

    lax.fori_loop(1, NG, produce, 0)

    eye256 = onehot(256, 256, lambda r: r)
    for t in range(4):
        for k in range(4):
            for h in range(2):
                rows = jnp.concatenate([jnp.concatenate(
                    [a_t[h, q, pl.ds((8 * t + 4 * gg + (m + k) % 4) * H, H), :] for gg in range(2) for m in range(4)],
                    axis=0) for q in range(HQ)], axis=1)
                block = dot(eye256, rows, NT).astype(BF16)
                for gg in range(2):
                    a_v[k, 2 * t + gg, HS * h:HS * h + HS, :] = block[:, 128 * gg:128 * gg + 128]

    w_copy.wait()
    w_f32[...] = w_buf[...].astype(F32)
    for d in range(H):
        block = w_f32[pl.ds(d, H, stride=H), :].astype(BF16)
        for v in range(4):
            w_v[v, pl.ds((d // 4) * 128 + ((v - d) % 4) * H, H), :] = block
    z_copy.wait()

    bias_out = bo_ref[...].astype(F32).reshape(1, Z)
    bias_ref[...] = jnp.broadcast_to(bias_out, (8, Z))
    def pair(slot_a, g_a, slot_b, g_b, k, h):
        return jnp.concatenate([jnp.concatenate(
            [b_buf[slot_a, g_a, h, q, KR * k:KR * k + KR, :], b_buf[slot_b, g_b, h, q, KR * k:KR * k + KR, :]],
            axis=0) for q in range(HQ)], axis=1)

    def outer(k, h, t, chunks):
        return dot(pair(*chunks, k, h), a_cols(a_v, k, t, HS * h, HS))

    def write(slot_a, g_a, slot_b, g_b):
        jc = (slot_a * NG + g_a, slot_b * NG + g_b)
        for v in range(4):
            u = project(lhs2, w_v, v) + bias_out
            for c in range(2):
                for G in range(8):
                    i = 4 * G + v
                    r0 = c * KR + G * J
                    out_ref[i, jc[c]] = (z_buf[i, jc[c]].astype(F32) + u[r0:r0 + J]).astype(BF16)

    def regroup_whole(*chunks):
        lhs = [jnp.concatenate([pair(*chunks, k, h) for h in range(2)], axis=1) for k in range(4)]
        regroup(lhs2, range(4), lambda k, t: dot(lhs[k], a_cols(a_v, k, t, 0, S)))

    def regroup_second(slot, part, steps):
        regroup(lhs2, steps, lambda k, t: part[k, :, 256 * t:256 * t + 256] + outer(k, 1, t, (slot, 2, slot, 3)))

    def unit(*chunks):
        regroup_whole(*chunks)
        write(*chunks)

    def local(s, _):
        slot = me + flip * (s // 2)
        g = 2 * (s % 2)

        @pl.when(s >= 2)
        def _():
            arrived(s % 2)

        unit(slot, g, slot, g + 1)
        return 0

    lax.fori_loop(0, 4, local, 0)

    def near(s, _):
        g = s // 2
        p = s % 2

        @pl.when(p == 0)
        def _():
            arrived(2 + g)
            for gc in range(NG):
                @pl.when(g == gc)
                def _():
                    slot, dev = (yn, xn) if gc % 2 == 0 else (xn, yn)
                    if gc < 2:
                        whole(slot, gc, dev, 10).start()
                    else:
                        @pl.when(core == 1)
                        def _():
                            half(slot, gc, 0, dev, 12).start()
                            half(slot, gc, 1, dev, 13).start()

                        @pl.when(core == 0)
                        def _():
                            half(slot, gc, 0, dev, 14).start()

            whole(xn, g, pt, 6 + g).start()
            whole(yn, g, pt, 6 + g).start()

        @pl.when(p == 1)
        def _():
            arrived(6 + g)

            @pl.when(core == 1)
            def _():
                @pl.when(g == 2)
                def _():
                    half(yn + flip, 2, 1, xn, 15).start()

                @pl.when(g == 3)
                def _():
                    half(xn + flip, 3, 1, yn, 15).start()

        unit(xn + flip * p, g, yn + flip * p, g)
        return 0

    lax.fori_loop(0, 2 * NG, near, 0)

    d1 = dg - core + 1
    d0 = dg - core

    def hand_on(slot, h, sem):
        half(slot, 2, h, pt, sem).start()
        half(slot, 3, h, pt, sem).start()

    def first_half(slot, part):
        for t in range(4):
            for k in range(4):
                part[k, :, 256 * t:256 * t + 256] = outer(k, 0, t, (slot, 2, slot, 3))

    def leave():
        for c in range(2):
            b_last[c] = b_buf[d0, 2 + c, 1]
        regroup_second(d0, part0, range(EARLY))

    def far_from():
        arrived(10)
        whole(dg, 0, pt, 11).start()
        whole(dg, 1, pt, 11).start()

    @pl.when(core == 1)
    def _():
        def far(q, _):
            @pl.when(q == 0)
            def _():
                far_from()

            @pl.when(q == 1)
            def _():
                arrived_halves(12)
                hand_on(d1, 0, 12)
                first_half(d1, part1)
                arrived(11)

            unit(d1 - q, 0, d1 - q, 1)
            return 0

        lax.fori_loop(0, 2, far, 0)
        arrived_halves(13)
        hand_on(d1, 1, 13)
        regroup_second(d1, part1, range(4))
        write(d1, 2, d1, 3)
        arrived_halves(15)
        hand_on(d0, 1, 15)
        arrived_halves(14)
        first_half(d0, part0)
        leave()

    @pl.when(core == 0)
    def _():
        def far(q, _):
            @pl.when(q == 0)
            def _():
                far_from()

            @pl.when(q == 1)
            def _():
                arrived(11)

            unit(d0 + q, 0, d0 + q, 1)
            return 0

        lax.fori_loop(0, 2, far, 0)

        arrived_halves(12)
        first_half(d1, part1)
        arrived_halves(14)
        hand_on(d0, 0, 14)
        first_half(d0, part0)
        arrived_halves(13)
        regroup_second(d1, part1, range(4))
        write(d1, 2, d1, 3)
        arrived_halves(15)
        leave()

    span(b_buf.at[pl.ds(0, 6)], 0, 0).wait_send()

    @pl.when(core == 1)
    def _():
        span(b_buf.at[pl.ds(0, 2), pl.ds(0, 3)], 1, 0).wait_send()

    @pl.when(core == 0)
    def _():
        span(b_buf.at[0, pl.ds(0, 2)], 1, 0).wait_send()


def last_kernel(out_ref, lhs2, w_v, z_buf, bias_ref, a_v, part0, b_last, out_hbm, later, tail, sem):
    me = lax.axis_index("dap")
    slot = 6 - me // 2 * 2
    for chip in range(4):
        @pl.when(me // 2 == chip)
        def _():
            hole = NG * (6 - 2 * chip) + 2
            for lo, n in ((0, hole), (hole + 2, N // J - hole - 2)):
                pltpu.make_async_copy(
                    out_ref.at[:, pl.ds(lo, n)], out_hbm.at[:, pl.ds(lo, n)], sem.at[0]).start()

    first = NG * slot + 2
    lhs = [jnp.concatenate([jnp.concatenate(
        [b_last[c, q, KR * k:KR * k + KR, :] for c in range(2)], axis=0) for q in range(HQ)], axis=1) for k in range(4)]
    regroup(later, range(EARLY, 4), lambda k, t: (
        part0[k, :, 256 * t:256 * t + 256] + dot(lhs[k], a_cols(a_v, k, t, HS, HS))))
    for v in range(4):
        u = project(lhs2, w_v, v, later) + bias_ref[:1, :]
        for c in range(2):
            for G in range(8):
                i = 4 * G + v
                r0 = c * KR + G * J
                tail[i, c] = (z_buf[i, first + c].astype(F32) + u[r0:r0 + J]).astype(BF16)
    rest = pltpu.make_async_copy(tail, out_hbm.at[:, pl.ds(first, 2)], sem.at[1])
    rest.start()
    done = out_ref.at[:, pl.ds(0, N // J - 2)]
    pltpu.make_async_copy(done, out_hbm.at[:, pl.ds(0, N // J - 2)], sem.at[0]).wait()
    rest.wait()


def local_update(z, m, lns, lno, wa, ba, wb, bb, wo, bo):
    hbm = pl.BlockSpec(memory_space=pltpu.HBM)
    vmem = pl.BlockSpec(memory_space=pltpu.VMEM)
    args = (z.reshape(NL, N // J, J, Z), m.transpose(1, 2, 0), lns.reshape(1, M), lno.reshape(1, M),
            wa.T, ba.reshape(1, H), wb.T, bb.reshape(1, H), wo, bo.reshape(1, Z))
    rows = jax.ShapeDtypeStruct((NL, N // J, J, Z), BF16)
    def scoped(*refs):
        pl.run_scoped(lambda in_sem, send_sem: kernel(*refs, in_sem, send_sem),
                      pltpu.SemaphoreType.DMA((14,)), pltpu.SemaphoreType.DMA((2,)))

    parts = pl.pallas_call(
        scoped,
        out_shape=(rows, jax.ShapeDtypeStruct((4, 8, 2 * KR, 128), BF16), jax.ShapeDtypeStruct((4, H * H, Z), BF16),
                   rows, jax.ShapeDtypeStruct((8, Z), F32), jax.ShapeDtypeStruct((4, NL * H // 128, S, 128), BF16),
                   jax.ShapeDtypeStruct((4, 2 * KR, NL * H), F32), jax.ShapeDtypeStruct((2, HQ, CR, 128), BF16)),
        in_specs=[hbm] * len(args),
        out_specs=(vmem,) * 8,
        scratch_shapes=[
            pltpu.VMEM((8, NG, 2, HQ, CR, 128), BF16),
            pltpu.VMEM((2, HQ, NL * H, 128), BF16),
            pltpu.VMEM((NL, M, S), BF16),
            pltpu.VMEM((HQ, CR, 128), F32),
            pltpu.VMEM((H * H, Z), BF16),
            pltpu.VMEM((H * H, Z), F32),
            pltpu.VMEM((3, M, 128), F32),
            pltpu.VMEM((1, M), BF16),
            pltpu.VMEM((1, M), BF16),
            pltpu.VMEM((H, M), BF16),
            pltpu.VMEM((1, H), BF16),
            pltpu.VMEM((H, M), BF16),
            pltpu.VMEM((1, H), BF16),
            pltpu.VMEM((1, Z), BF16),
            pltpu.VMEM((4, 2 * KR, NL * H), F32),
            pltpu.SemaphoreType.DMA((16,)),
        ],
        compiler_params=pltpu.CompilerParams(
            collective_id=0, has_side_effects=True, vmem_limit_bytes=28 * 1024 * 1024),
    )(*(pltpu.with_memory_space_constraint(x, pltpu.HBM) for x in args))
    out = pl.pallas_call(
        last_kernel,
        out_shape=rows,
        in_specs=[vmem] * 8,
        out_specs=hbm,
        scratch_shapes=[pltpu.VMEM((4, 8, 2 * KR, 128), BF16), pltpu.VMEM((NL, 2, J, Z), BF16),
                        pltpu.SemaphoreType.DMA((2,))],
        compiler_params=pltpu.CompilerParams(vmem_limit_bytes=6 * 1024 * 1024),
    )(*parts)
    return out.reshape(NL, N, Z)


def solution(mesh):
    row, col, rep = P(("batch", "dap")), P(None, ("batch", "dap")), P()
    return jax.shard_map(local_update, mesh=mesh, in_specs=(row, col) + (rep,) * 8, out_specs=row, check_vma=False)
```

```python
import jax
import jax.numpy as jnp
from jax import lax
from jax.experimental import pallas as pl
from jax.experimental.pallas import tpu as pltpu
from jax.sharding import PartitionSpec as P

MESH = pl.DeviceIdType.MESH
F32, BF16 = jnp.float32, jnp.bfloat16
LN_EPS = 1e-5
S, NL, M, H, N, Z = 512, 32, 64, 32, 256, 128
J = 8
NG = NL // J
CR = H * J
KR = CR // 4
HS = S // 2
EARLY = 2
HQ = HS // 128
NT = (((1,), (1,)), ((), ()))
NN = (((1,), (0,)), ((), ()))


def dot(x, y, dims=NN):
    return lax.dot_general(x, y, dims, preferred_element_type=F32)


def onehot(rows, cols, fn):
    r = lax.broadcasted_iota(jnp.int32, (rows, cols), 0)
    c = lax.broadcasted_iota(jnp.int32, (rows, cols), 1)
    return jnp.where(fn(r) == c, 1.0, 0.0).astype(BF16)


def a_cols(a_v, k, t, lo, n):
    return jnp.concatenate([a_v[k, 2 * t + gg, lo:lo + n, :] for gg in range(2)], axis=1)


def regroup(lhs2, steps, product):
    lane = lax.broadcasted_iota(jnp.int32, (2 * KR, 128), 1) // H
    even = lane % 2 == 0
    ends = (lane == 0) | (lane == 3)
    low = lane < 2
    for t in steps:
        o = [product(k, t) * (1.0 / S) for k in range(4)]
        q = [[None, None] for _ in range(4)]
        for gg in range(2):
            p = [x[:, 128 * gg:128 * gg + 128] for x in o]
            e0, f0 = jnp.where(even, p[0], p[1]), jnp.where(even, p[2], p[3])
            e1, f1 = jnp.where(even, p[1], p[0]), jnp.where(even, p[3], p[2])
            q[0][gg] = jnp.where(ends, e0, f0)
            q[2][gg] = jnp.where(ends, f0, e0)
            q[1][gg] = jnp.where(low, e1, f1)
            q[3][gg] = jnp.where(low, f1, e1)
        for v in range(4):
            for c in range(2):
                for e in range(8):
                    r0 = c * KR + e * J
                    lhs2[v, e, c * KR + 16 * t:c * KR + 16 * t + 16, :] = jnp.concatenate(
                        [q[v][0][r0:r0 + J], q[v][1][r0:r0 + J]], axis=0).astype(BF16)


def project(lhs2, w_v, v, later=None):
    def rows(e):
        if later is None:
            return lhs2[v, e]
        return jnp.concatenate([x for c in range(2) for x in (
            lhs2[v, e, c * KR:c * KR + 16 * EARLY, :], later[v, e, c * KR + 16 * EARLY:c * KR + KR, :])], axis=0)

    return dot(jnp.concatenate([rows(e) for e in range(8)], axis=1), w_v[v])


def kernel(z_hbm, m_hbm, lns_hbm, lno_hbm, wa_hbm, ba_hbm, wb_hbm, bb_hbm, wo_hbm, bo_hbm,
           out_ref, lhs2, w_v, z_buf, bias_ref, a_v, part0, b_last,
           b_buf, a_t, m_buf, b_f32, w_buf, w_f32, par,
           lns_ref, lno_ref, wa_ref, ba_ref, wb_ref, bb_ref, bo_ref,
           part1, recv_sem, in_sem, send_sem):
    me = lax.axis_index("dap")
    core = me % 2
    xbit = (me // 2) % 2
    pt = me + 1 - 2 * core
    flip = pt - me
    xn = me + 2 - 4 * xbit
    yn = (me + 4) % 8
    dg = (xn + 4) % 8

    barrier = pltpu.get_barrier_semaphore()
    for dev in (pt, xn, yn):
        pl.semaphore_signal(barrier, inc=1, device_id={"dap": dev}, device_id_type=MESH)

    def m_part(i):
        part_of = pl.ds(0, J), slice(None), pl.ds(i * 128, 128)
        return pltpu.make_async_copy(m_hbm.at[part_of], m_buf.at[part_of], in_sem.at[i])

    m_rest = pltpu.make_async_copy(m_hbm.at[pl.ds(J, NL - J)], m_buf.at[pl.ds(J, NL - J)], in_sem.at[12])
    w_copy = pltpu.make_async_copy(wo_hbm, w_buf, in_sem.at[13])
    z_copy = pltpu.make_async_copy(z_hbm, z_buf, in_sem.at[4])
    small = [pltpu.make_async_copy(src, dst, in_sem.at[5 + i]) for i, (src, dst) in enumerate((
        (lns_hbm, lns_ref), (lno_hbm, lno_ref), (wa_hbm, wa_ref), (ba_hbm, ba_ref),
        (wb_hbm, wb_ref), (bb_hbm, bb_ref), (bo_hbm, bo_ref)))]
    for copy in small:
        copy.start()
    for n in range(0, J, 2):
        part_of = pl.ds(n, 2), slice(None), pl.ds(0, 128)
        pltpu.make_async_copy(m_hbm.at[part_of], m_buf.at[part_of], in_sem.at[0]).start()
    for i in range(1, S // 128):
        m_part(i).start()

    def whole(slot, g, dev, sem):
        return pltpu.make_async_remote_copy(
            src_ref=b_buf.at[slot, g], dst_ref=b_buf.at[slot, g], send_sem=send_sem.at[0],
            recv_sem=recv_sem.at[sem], device_id={"dap": dev}, device_id_type=MESH)

    def half(slot, g, h, dev, sem, k=1):
        return pltpu.make_async_remote_copy(
            src_ref=b_buf.at[slot, g, h], dst_ref=b_buf.at[slot, g, h], send_sem=send_sem.at[k],
            recv_sem=recv_sem.at[sem], device_id={"dap": dev}, device_id_type=MESH)

    def span(ref, k, sem):
        return pltpu.make_async_remote_copy(
            src_ref=ref, dst_ref=ref, send_sem=send_sem.at[k], recv_sem=recv_sem.at[sem],
            device_id={"dap": pt}, device_id_type=MESH)

    def arrived(sem):
        span(b_buf.at[0, pl.ds(0, 2)], 0, sem).wait_recv()

    def arrived_halves(sem):
        span(b_buf.at[0, 0], 0, sem).wait_recv()

    for copy in small:
        copy.wait()

    def column(row, width):
        return jnp.broadcast_to(row.astype(F32).reshape(1, width), (128, width)).astype(BF16)

    eye = onehot(M, M, lambda r: r)
    order = onehot(2 * H, 2 * H, lambda r: jnp.where(r < H, r, H + 4 * ((r - H) % 8) + (r - H) // 8))
    w_ab = dot(order, jnp.concatenate([wa_ref[...], wb_ref[...]], axis=0)).astype(BF16)
    par[0] = dot(eye, column(lns_ref[...], M), NT)
    par[1] = dot(eye, column(lno_ref[...], M), NT)
    bias = jnp.concatenate([column(ba_ref[...], H), column(bb_ref[...], H)], axis=1)
    par[2] = dot(order, bias, NT)

    def make(g, h, q0, nq):
        def lanes(i):
            return jnp.concatenate([par[i]] * nq, axis=1)

        lo = HS * h + 128 * q0
        for n in range(J):
            x = m_buf[g * J + n, :, lo:lo + 128 * nq].astype(F32)
            mean = jnp.sum(x, axis=0, keepdims=True) * (1.0 / M)
            x = x - mean
            var = jnp.sum(x * x, axis=0, keepdims=True) * (1.0 / M)
            x = x * lax.rsqrt(var + LN_EPS)
            x = (x * lanes(0) + lanes(1)).astype(BF16)
            r = dot(w_ab, x) + lanes(2)
            for q in range(nq):
                rq = r[:, 128 * q:128 * q + 128]
                a_t[h, q0 + q, pl.ds((g * J + n) * H, H), :] = rq[:H].astype(BF16)
                b_f32[q0 + q, pl.ds(n, H, stride=J), :] = rq[H:]
        for q in range(q0, q0 + nq):
            b_buf[me, g, h, q] = b_f32[q].astype(BF16)

    for i in range(S // 128):
        m_part(i).wait()
        if i == 0:
            m_rest.start()
            w_copy.start()
            z_copy.start()
        h, q = i // HQ, i % HQ
        make(0, h, q, 1)
        if i == 0:
            pl.semaphore_wait(barrier, 3)
        for dev, sem in ((xn, 2), (yn, 2), (pt, 0)):
            piece = b_buf.at[me, 0, h, q]
            pltpu.make_async_remote_copy(
                src_ref=piece, dst_ref=piece, send_sem=send_sem.at[0], recv_sem=recv_sem.at[sem],
                device_id={"dap": dev}, device_id_type=MESH).start()
    m_rest.wait()

    def produce(g, _):
        for h in range(2):
            make(g, h, 0, HQ)
        whole(me, g, xn, 2 + g).start()
        whole(me, g, yn, 2 + g).start()
        whole(me, g, pt, 0).start()
        return 0

    lax.fori_loop(1, NG, produce, 0)

    eye256 = onehot(256, 256, lambda r: r)
    for t in range(4):
        for k in range(4):
            for h in range(2):
                rows = jnp.concatenate([jnp.concatenate(
                    [a_t[h, q, pl.ds((8 * t + 4 * gg + (m + k) % 4) * H, H), :] for gg in range(2) for m in range(4)],
                    axis=0) for q in range(HQ)], axis=1)
                block = dot(eye256, rows, NT).astype(BF16)
                for gg in range(2):
                    a_v[k, 2 * t + gg, HS * h:HS * h + HS, :] = block[:, 128 * gg:128 * gg + 128]

    w_copy.wait()
    w_f32[...] = w_buf[...].astype(F32)
    for d in range(H):
        block = w_f32[pl.ds(d, H, stride=H), :].astype(BF16)
        for v in range(4):
            w_v[v, pl.ds((d // 4) * 128 + ((v - d) % 4) * H, H), :] = block
    z_copy.wait()

    bias_out = bo_ref[...].astype(F32).reshape(1, Z)
    bias_ref[...] = jnp.broadcast_to(bias_out, (8, Z))
    def pair(slot_a, g_a, slot_b, g_b, k, h):
        return jnp.concatenate([jnp.concatenate(
            [b_buf[slot_a, g_a, h, q, KR * k:KR * k + KR, :], b_buf[slot_b, g_b, h, q, KR * k:KR * k + KR, :]],
            axis=0) for q in range(HQ)], axis=1)

    def outer(k, h, t, chunks):
        return dot(pair(*chunks, k, h), a_cols(a_v, k, t, HS * h, HS))

    def write(slot_a, g_a, slot_b, g_b):
        jc = (slot_a * NG + g_a, slot_b * NG + g_b)
        for v in range(4):
            u = project(lhs2, w_v, v) + bias_out
            for c in range(2):
                for G in range(8):
                    i = 4 * G + v
                    r0 = c * KR + G * J
                    out_ref[i, jc[c]] = (z_buf[i, jc[c]].astype(F32) + u[r0:r0 + J]).astype(BF16)

    def regroup_whole(*chunks):
        lhs = [jnp.concatenate([pair(*chunks, k, h) for h in range(2)], axis=1) for k in range(4)]
        regroup(lhs2, range(4), lambda k, t: dot(lhs[k], a_cols(a_v, k, t, 0, S)))

    def regroup_second(slot, part, steps):
        regroup(lhs2, steps, lambda k, t: part[k, :, 256 * t:256 * t + 256] + outer(k, 1, t, (slot, 2, slot, 3)))

    def unit(*chunks):
        regroup_whole(*chunks)
        write(*chunks)

    def local(s, _):
        slot = me + flip * (s // 2)
        g = 2 * (s % 2)

        @pl.when(s == 2)
        def _():
            span(b_buf.at[0], 0, 0).wait_recv()

        unit(slot, g, slot, g + 1)
        return 0

    lax.fori_loop(0, 4, local, 0)

    def near(s, _):
        g = s // 2
        p = s % 2

        @pl.when(p == 0)
        def _():
            arrived(2 + g)
            for gc in range(NG):
                @pl.when(g == gc)
                def _():
                    slot, dev = (yn, xn) if gc % 2 == 0 else (xn, yn)
                    if gc < 2:
                        whole(slot, gc, dev, 10).start()
                    else:
                        @pl.when(core == 1)
                        def _():
                            half(slot, gc, 0, dev, 12).start()
                            half(slot, gc, 1, dev, 13).start()

                        @pl.when(core == 0)
                        def _():
                            half(slot, gc, 0, dev, 14).start()

            whole(xn, g, pt, 6 + g).start()
            whole(yn, g, pt, 6 + g).start()

        @pl.when(p == 1)
        def _():
            arrived(6 + g)

            @pl.when(core == 1)
            def _():
                @pl.when(g == 2)
                def _():
                    half(yn + flip, 2, 1, xn, 15).start()

                @pl.when(g == 3)
                def _():
                    half(xn + flip, 3, 1, yn, 1).start()

        unit(xn + flip * p, g, yn + flip * p, g)
        return 0

    lax.fori_loop(0, 2 * NG, near, 0)

    d1 = dg - core + 1
    d0 = dg - core

    def hand_on(slot, h, sem):
        half(slot, 2, h, pt, sem).start()
        half(slot, 3, h, pt, sem).start()

    def first_half(slot, part):
        for t in range(4):
            for k in range(4):
                part[k, :, 256 * t:256 * t + 256] = outer(k, 0, t, (slot, 2, slot, 3))

    def leave():
        for c in range(2):
            b_last[c] = b_buf[d0, 2 + c, 1]
        regroup_second(d0, part0, range(EARLY))

    def far_from():
        arrived(10)
        whole(dg, 0, pt, 11).start()
        whole(dg, 1, pt, 11).start()

    @pl.when(core == 1)
    def _():
        def far(q, _):
            @pl.when(q == 0)
            def _():
                far_from()

            @pl.when(q == 1)
            def _():
                arrived_halves(12)
                hand_on(d1, 0, 12)
                first_half(d1, part1)
                arrived(11)

            unit(d1 - q, 0, d1 - q, 1)
            return 0

        lax.fori_loop(0, 2, far, 0)
        arrived_halves(13)
        hand_on(d1, 1, 13)
        regroup_second(d1, part1, range(4))
        write(d1, 2, d1, 3)
        for g in (2, 3):
            span(b_buf.at[0, 0, 0], 0, 15 if g == 2 else 1).wait_recv()
            half(d0, g, 1, pt, 15).start()
        arrived_halves(14)
        first_half(d0, part0)
        leave()

    @pl.when(core == 0)
    def _():
        def far(q, _):
            @pl.when(q == 0)
            def _():
                far_from()

            @pl.when(q == 1)
            def _():
                arrived(11)

            unit(d0 + q, 0, d0 + q, 1)
            return 0

        lax.fori_loop(0, 2, far, 0)

        arrived_halves(12)
        first_half(d1, part1)
        arrived_halves(14)
        hand_on(d0, 0, 14)
        first_half(d0, part0)
        arrived_halves(13)
        regroup_second(d1, part1, range(4))
        write(d1, 2, d1, 3)
        arrived_halves(15)
        leave()

    span(b_buf.at[pl.ds(0, 6)], 0, 0).wait_send()

    @pl.when(core == 1)
    def _():
        span(b_buf.at[pl.ds(0, 2), pl.ds(0, 3)], 1, 0).wait_send()

    @pl.when(core == 0)
    def _():
        span(b_buf.at[0, pl.ds(0, 2)], 1, 0).wait_send()


def last_kernel(out_ref, lhs2, w_v, z_buf, bias_ref, a_v, part0, b_last, out_hbm, later, tail, sem):
    me = lax.axis_index("dap")
    slot = 6 - me // 2 * 2
    for chip in range(4):
        @pl.when(me // 2 == chip)
        def _():
            hole = NG * (6 - 2 * chip) + 2
            for lo, n in ((0, hole), (hole + 2, N // J - hole - 2)):
                pltpu.make_async_copy(
                    out_ref.at[:, pl.ds(lo, n)], out_hbm.at[:, pl.ds(lo, n)], sem.at[0]).start()

    first = NG * slot + 2
    lhs = [jnp.concatenate([jnp.concatenate(
        [b_last[c, q, KR * k:KR * k + KR, :] for c in range(2)], axis=0) for q in range(HQ)], axis=1) for k in range(4)]
    regroup(later, range(EARLY, 4), lambda k, t: (
        part0[k, :, 256 * t:256 * t + 256] + dot(lhs[k], a_cols(a_v, k, t, HS, HS))))
    for v in range(4):
        u = project(lhs2, w_v, v, later) + bias_ref[:1, :]
        for c in range(2):
            for G in range(8):
                i = 4 * G + v
                r0 = c * KR + G * J
                tail[i, c] = (z_buf[i, first + c].astype(F32) + u[r0:r0 + J]).astype(BF16)
    rest = pltpu.make_async_copy(tail, out_hbm.at[:, pl.ds(first, 2)], sem.at[1])
    rest.start()
    done = out_ref.at[:, pl.ds(0, N // J - 2)]
    pltpu.make_async_copy(done, out_hbm.at[:, pl.ds(0, N // J - 2)], sem.at[0]).wait()
    rest.wait()


def local_update(z, m, lns, lno, wa, ba, wb, bb, wo, bo):
    hbm = pl.BlockSpec(memory_space=pltpu.HBM)
    vmem = pl.BlockSpec(memory_space=pltpu.VMEM)
    args = (z.reshape(NL, N // J, J, Z), m.transpose(1, 2, 0), lns.reshape(1, M), lno.reshape(1, M),
            wa.T, ba.reshape(1, H), wb.T, bb.reshape(1, H), wo, bo.reshape(1, Z))
    rows = jax.ShapeDtypeStruct((NL, N // J, J, Z), BF16)
    def scoped(*refs):
        pl.run_scoped(lambda in_sem, send_sem: kernel(*refs, in_sem, send_sem),
                      pltpu.SemaphoreType.DMA((14,)), pltpu.SemaphoreType.DMA((2,)))

    parts = pl.pallas_call(
        scoped,
        out_shape=(rows, jax.ShapeDtypeStruct((4, 8, 2 * KR, 128), BF16), jax.ShapeDtypeStruct((4, H * H, Z), BF16),
                   rows, jax.ShapeDtypeStruct((8, Z), F32), jax.ShapeDtypeStruct((4, NL * H // 128, S, 128), BF16),
                   jax.ShapeDtypeStruct((4, 2 * KR, NL * H), F32), jax.ShapeDtypeStruct((2, HQ, CR, 128), BF16)),
        in_specs=[hbm] * len(args),
        out_specs=(vmem,) * 8,
        scratch_shapes=[
            pltpu.VMEM((8, NG, 2, HQ, CR, 128), BF16),
            pltpu.VMEM((2, HQ, NL * H, 128), BF16),
            pltpu.VMEM((NL, M, S), BF16),
            pltpu.VMEM((HQ, CR, 128), F32),
            pltpu.VMEM((H * H, Z), BF16),
            pltpu.VMEM((H * H, Z), F32),
            pltpu.VMEM((3, M, 128), F32),
            pltpu.VMEM((1, M), BF16),
            pltpu.VMEM((1, M), BF16),
            pltpu.VMEM((H, M), BF16),
            pltpu.VMEM((1, H), BF16),
            pltpu.VMEM((H, M), BF16),
            pltpu.VMEM((1, H), BF16),
            pltpu.VMEM((1, Z), BF16),
            pltpu.VMEM((4, 2 * KR, NL * H), F32),
            pltpu.SemaphoreType.DMA((16,)),
        ],
        compiler_params=pltpu.CompilerParams(
            collective_id=0, has_side_effects=True, vmem_limit_bytes=28 * 1024 * 1024),
    )(*(pltpu.with_memory_space_constraint(x, pltpu.HBM) for x in args))
    out = pl.pallas_call(
        last_kernel,
        out_shape=rows,
        in_specs=[vmem] * 8,
        out_specs=hbm,
        scratch_shapes=[pltpu.VMEM((4, 8, 2 * KR, 128), BF16), pltpu.VMEM((NL, 2, J, Z), BF16),
                        pltpu.SemaphoreType.DMA((2,))],
        compiler_params=pltpu.CompilerParams(vmem_limit_bytes=6 * 1024 * 1024),
    )(*parts)
    return out.reshape(NL, N, Z)


def solution(mesh):
    row, col, rep = P(("batch", "dap")), P(None, ("batch", "dap")), P()
    return jax.shard_map(local_update, mesh=mesh, in_specs=(row, col) + (rep,) * 8, out_specs=row, check_vma=False)
```
